32 devices in a mesh: freq: 8 (over z, x), tm: 4 (over y, core).
Axes of the slice: x: 2, y: 2, z: 4, core: 2. Of those that a mesh axis runs over, the one named last changes fastest.
Arguments:
- vis: bfloat16 [16, 8, 16, 2, 128, 128], P('freq', 'tm'), may hold values from -6 to 6
- model: bfloat16 [16, 8, 16, 2, 128, 128], P('freq', 'tm'), may hold values from -6 to 6
- block_rows: int32 [16, 8, 16], P('freq', 'tm'), may hold values from 0 to 15
- block_cols: int32 [16, 8, 16], P('freq', 'tm'), may hold values from 0 to 15
- flags: int32 [16, 8, 16], P('freq', 'tm'), may hold values 0 or 1
- prior: float32 [16, 8, 2, 2048], P('freq', 'tm'), may hold values from -6 to 6
- couplings: float32 [3, 2048], replicated, may hold values from 0.1 to 0.6
- damping: float32 [2048], replicated, may hold values from 8 to 128
Outputs:
- gains: float32 [16, 8, 2, 2048], P('freq', 'tm')
- changes: float32 [4], replicated
The draws below stay inside these ranges and needn't reach their ends.
All inputs are finite; a program needn't handle non-finite values. No bound on the sum of `flags` on one device may be relied on, other than what follows from the above.
Results may differ from the reference program's by a relative error of at most 0.0003.
Values sent between devices are 32-bit elements; how exact they have to be, the bound alone decides.
A program may use at most 64 MiB of HBM per device.

```python
import math
import jax
import jax.numpy as jnp
from jax import lax

N = 2048
BS = 128
NB = 16
BLK = 16
ITERS = 4
FREQ = 16
TIMES = 8


def place_ends(result, stream_key, low, top_value):
    index_at = [jax.random.randint(jax.random.fold_in(stream_key, axis), (), 0, length) for axis, length in enumerate(result.shape)]
    longest = result.shape.index(max(result.shape))
    neighbour = index_at[:longest] + [(index_at[longest] + 1) % result.shape[longest]] + index_at[longest + 1:]
    return result.at[tuple(index_at)].set(low).at[tuple(neighbour)].set(top_value)


def block_scale(stream_key, dims, pieces, least, top_value):
    def one(axis_at, shards_of):
        heights = jax.random.uniform(jax.random.fold_in(jax.random.fold_in(stream_key, 6), axis_at), (shards_of,), jnp.float32, least / len(pieces), top_value / len(pieces))
        return jnp.repeat(jnp.exp(heights), dims[axis_at] // shards_of).reshape((-1,) + (1,) * (len(dims) - axis_at - 1))

    level = one(*pieces[0])
    for cut in pieces[1:]:
        level = level * one(*cut)
    return level


def centred(key, dims, scale, reach, pieces=(), held_as=jnp.bfloat16):
    result = jax.random.normal(key, dims, jnp.float32) * scale
    if len(pieces) > 0:
        result = block_scale(key, dims, pieces, -0.22, 0.18) * result
    return jnp.clip(result, min=-reach, max=reach).astype(held_as)


def setup_inputs(seed: int = 0) -> dict:
    seeds = jax.random.split(jax.random.key(seed), 9)
    vis = centred(seeds[0], (FREQ, TIMES, BLK, 2, BS, BS), 1.0, 6.0, ((0, 8), (1, 4)))
    model = centred(seeds[1], (FREQ, TIMES, BLK, 2, BS, BS), 1.0, 6.0, ((0, 8), (1, 4)))
    block_rows = place_ends(jax.random.randint(seeds[2], (FREQ, TIMES, BLK), 0, NB), jax.random.fold_in(seeds[2], 1), 0, NB - 1).astype(jnp.int32)
    block_cols = place_ends(jax.random.randint(seeds[3], (FREQ, TIMES, BLK), 0, NB), jax.random.fold_in(seeds[3], 1), 0, NB - 1).astype(jnp.int32)
    flags = place_ends((jax.random.randint(seeds[4], (FREQ, TIMES, BLK), 0, 4) < 3).astype(jnp.int32), jax.random.fold_in(seeds[4], 1), 0, 1)
    prior = centred(seeds[5], (FREQ, TIMES, 2, N), 1.0, 6.0, ((0, 8), (1, 4)), jnp.float32)
    couplings = jnp.clip(jnp.exp(jax.random.uniform(seeds[6], (3, N), jnp.float32, math.log(0.1), math.log(0.6))), 0.1, 0.6)
    damping = jnp.clip(jnp.exp(jax.random.uniform(seeds[7], (N,), jnp.float32, math.log(8.0), math.log(128.0))), 8.0, 128.0)
    return {"vis": vis, "model": model, "block_rows": block_rows, "block_cols": block_cols, "flags": flags, "prior": prior, "couplings": couplings, "damping": damping}


def tile_terms(gains, rows, cols, flags, vis, model):
    width = vis.shape[-1]
    blocks = gains.shape[-1] // width
    count = gains.shape[0]
    gain_blocks = gains.reshape(count, 2, blocks, width)
    labels = jnp.arange(blocks, dtype=jnp.int32)
    row_hot = (rows[..., None] == labels).astype(jnp.float32)
    col_hot = (cols[..., None] == labels).astype(jnp.float32)
    row_gain = jnp.einsum('kbn,kcnr->kbcr', row_hot, gain_blocks, precision=lax.Precision.HIGHEST)
    grow_re = row_gain[:, :, 0][..., None]
    grow_im = row_gain[:, :, 1][..., None]
    model_re = model[:, :, 0].astype(jnp.float32)
    model_im = model[:, :, 1].astype(jnp.float32)
    vis_re = vis[:, :, 0].astype(jnp.float32)
    vis_im = vis[:, :, 1].astype(jnp.float32)
    zeta_re = grow_re * model_re - grow_im * model_im
    zeta_im = grow_re * model_im + grow_im * model_re
    num_re = lax.optimization_barrier(jnp.sum(vis_re * zeta_re + vis_im * zeta_im, axis=-2))
    num_im = lax.optimization_barrier(jnp.sum(vis_re * zeta_im - vis_im * zeta_re, axis=-2))
    denom = lax.optimization_barrier(jnp.sum(zeta_re * zeta_re + zeta_im * zeta_im, axis=-2))
    terms = jnp.stack([num_re, num_im, denom], axis=2) * flags.astype(jnp.float32)[..., None, None]
    summed = jnp.einsum('kbn,kbcr->kcnr', col_hot, terms, precision=lax.Precision.HIGHEST)
    return summed.reshape(count, 3, blocks * width)

def reference(vis, model, block_rows, block_cols, flags, prior, couplings, damping):
    prior_prev = jnp.roll(prior, 1, axis=0)
    current = prior
    changes = []
    for step in range(ITERS):
        terms = lax.map(lambda items: tile_terms(*items), (current, block_rows, block_cols, flags, vis, model))
        near = jnp.roll(terms, 1, axis=0) + jnp.roll(terms, -1, axis=0)
        far = jnp.roll(terms, 2, axis=0) + jnp.roll(terms, -2, axis=0)
        padded = jnp.pad(terms, ((0, 0), (1, 1), (0, 0), (0, 0)))
        later = padded[:, :-2] + padded[:, 2:]
        smooth = terms + couplings[0] * near + couplings[1] * far + couplings[2] * later
        numer = smooth[:, :, 0:2] + damping * prior_prev
        denom = smooth[:, :, 2] + damping
        fresh = numer / denom[:, :, None]
        if step % 2 == 1:
            fresh = 0.5 * (fresh + current)
        change = jnp.sum((fresh - current) ** 2)
        scale = jnp.sum(fresh * fresh)
        changes.append(jnp.sqrt(change / (scale + 1e-06)))
        current = fresh
    return (current, jnp.stack(changes))
```

```python
import functools

import jax
import jax.numpy as jnp
from jax import lax
from jax.experimental import pallas as pl
from jax.experimental.pallas import tpu as pltpu
from jax.sharding import PartitionSpec as P

ITERS = 4
REACH = 2
MESH = pl.DeviceIdType.MESH
F32 = jnp.float32
BF16 = jnp.bfloat16


def split(value):
    high = value.astype(BF16)
    return high, (value - high.astype(F32)).astype(BF16)


def kernel(
    dims,
    vis_ref, model_ref, rows_in, cols_in, flags_in, prior_in, coup_in, damp_in,
    gains_ref, changes_ref,
    rows_ref, cols_ref, flags_ref, prior_ref, coup_ref, damp_ref,
    vbuf, mbuf, wa, wb, gain, prev, coef, from_prior, terms, low, high, early, late,
    stats, all_stats,
    small_sem, load_sem, prior_sem, up_send, down_send, low_recv, high_recv,
    early_send, late_send, early_recv, late_recv, stats_send, stats_recv,
):
    nf, nt, ftiles, ttiles, blks, width, nb = dims
    fi = lax.axis_index("freq")
    ti = lax.axis_index("tm")
    above, below = lax.rem(fi + 1, nf), lax.rem(fi + nf - 1, nf)
    tiles = [(f, t) for t in range(ttiles) for f in range(ftiles)]

    def at_tile(f, t):
        return t * ftiles + f

    devices = nf * nt
    me = fi * nt + ti

    def peer(step):
        other = lax.rem(me + step, devices)
        return other, {"freq": other // nt, "tm": lax.rem(other, nt)}

    small = [
        pltpu.make_async_copy(src, dst, small_sem.at[n])
        for n, (src, dst) in enumerate((
            (prior_in, prior_ref), (coup_in, coup_ref), (damp_in, damp_ref),
            (rows_in, rows_ref), (cols_in, cols_ref), (flags_in, flags_ref),
        ))
    ]
    for copy in small:
        copy.start()

    def loads(f, t):
        i = at_tile(f, t)
        return (
            pltpu.make_async_copy(vis_ref.at[f, t], vbuf.at[i], load_sem.at[0, i]),
            pltpu.make_async_copy(model_ref.at[f, t], mbuf.at[i], load_sem.at[1, i]),
        )

    for f, t in tiles:
        for copy in loads(f, t):
            copy.start()

    barrier = pltpu.get_barrier_semaphore()

    def greet(step, carry):
        pl.semaphore_signal(barrier, inc=1, device_id=peer(step)[1], device_id_type=MESH)
        return carry

    lax.fori_loop(1, devices, greet, 0)
    for copy in small:
        copy.wait()

    for f, t in tiles:
        i = at_tile(f, t)
        for c in range(2):
            for n in range(nb):
                gain[i, c, n : n + 1, :] = prior_ref[f, t, c : c + 1, n * width : (n + 1) * width]
    for n in range(nb):
        for c in range(3):
            coef[c, n : n + 1, :] = coup_ref[c : c + 1, n * width : (n + 1) * width]
        coef[3, n : n + 1, :] = damp_ref[0:1, n * width : (n + 1) * width]

    prior_copy = pltpu.make_async_remote_copy(
        src_ref=prior_ref.at[ftiles - 1], dst_ref=from_prior,
        send_sem=prior_sem.at[0], recv_sem=prior_sem.at[1],
        device_id={"freq": above}, device_id_type=MESH,
    )

    def up_copy(k, f, t):
        s = t * REACH + f - (ftiles - REACH)
        return pltpu.make_async_remote_copy(
            src_ref=terms.at[k, at_tile(f, t)], dst_ref=low.at[k, s],
            send_sem=up_send.at[k, s], recv_sem=low_recv.at[k, s],
            device_id={"freq": above}, device_id_type=MESH,
        )

    def down_copy(k, f, t):
        s = t * REACH + f
        return pltpu.make_async_remote_copy(
            src_ref=terms.at[k, at_tile(f, t)], dst_ref=high.at[k, s],
            send_sem=down_send.at[k, s], recv_sem=high_recv.at[k, s],
            device_id={"freq": below}, device_id_type=MESH,
        )

    def later_copy(k, f):
        return pltpu.make_async_remote_copy(
            src_ref=terms.at[k, at_tile(f, ttiles - 1)], dst_ref=early.at[k, f],
            send_sem=early_send.at[k, f], recv_sem=early_recv.at[k, f],
            device_id={"tm": lax.rem(ti + 1, nt)}, device_id_type=MESH,
        )

    def earlier_copy(k, f):
        return pltpu.make_async_remote_copy(
            src_ref=terms.at[k, at_tile(f, 0)], dst_ref=late.at[k, f],
            send_sem=late_send.at[k, f], recv_sem=late_recv.at[k, f],
            device_id={"tm": lax.rem(ti + nt - 1, nt)}, device_id_type=MESH,
        )

    def prepare(i):
        def pair(p, carry):
            for side in range(2):
                b = 2 * p + side
                lo = side * width
                v_re = vbuf[i, b, 0].astype(F32)
                v_im = vbuf[i, b, 1].astype(F32)
                m_re = mbuf[i, b, 0].astype(F32)
                m_im = mbuf[i, b, 1].astype(F32)
                re_hi, re_lo = split(v_re * m_re + v_im * m_im)
                im_hi, im_lo = split(v_re * m_im - v_im * m_re)
                sq_hi, sq_lo = split(m_re * m_re + m_im * m_im)
                wa[i * blks + b, 0:width, 0:width] = re_hi
                wa[i * blks + b, width:, 0:width] = im_hi
                wa[i * blks + b, 0:width, width:] = sq_hi
                wa[i * blks + b, width:, width:] = sq_lo
                wb[i * (blks // 2) + p, 0:width, lo : lo + width] = re_lo
                wb[i * (blks // 2) + p, width:, lo : lo + width] = im_lo
            return carry

        lax.fori_loop(0, blks // 2, pair, 0)

    row_of = lax.broadcasted_iota(jnp.int32, (8, width), 0)
    block_of = lax.broadcasted_iota(jnp.int32, (nb, width), 0)

    def tile_terms(k, f, t):
        i = at_tile(f, t)
        total = [jnp.zeros((nb, width), F32) for _ in range(3)]
        for p in range(blks // 2):
            highs, outs, cols = [], [], []
            for b in (2 * p, 2 * p + 1):
                row = rows_ref[f, t, b]
                cols.append(jnp.where(flags_ref[f, t, b] != 0, cols_ref[f, t, b], -1))
                re = jnp.broadcast_to(gain[i, 0, pl.ds(row, 1), :], (8, width))
                im = jnp.broadcast_to(gain[i, 1, pl.ds(row, 1), :], (8, width))
                sq = re * re + im * im
                left = jnp.where(row_of == 0, re, jnp.where(row_of == 1, im, sq))
                right = jnp.where(row_of == 0, -im, jnp.where(row_of == 1, re, sq))
                lhs = jnp.concatenate([left, right], axis=1)
                lhs_hi = lhs.astype(BF16).astype(F32)
                highs.append(lhs_hi)
                lhs = jnp.concatenate([lhs_hi, lhs - lhs_hi], axis=0).astype(BF16)
                out = jnp.dot(lhs, wa[i * blks + b], preferred_element_type=F32)
                outs.append(out[0:8] + out[8:16])
            low_out = jnp.dot(
                jnp.concatenate(highs, axis=0).astype(BF16),
                wb[i * (blks // 2) + p],
                preferred_element_type=F32,
            )
            low_outs = (low_out[0:8, 0:width], low_out[8:16, width:])
            for out, low_out, col in zip(outs, low_outs, cols):
                num = out[:, 0:width] + low_out
                den = out[:, width:]
                hit = block_of == col
                parts = (num[0:1], num[1:2], den[2:3])
                total = [
                    acc + jnp.where(hit, jnp.broadcast_to(one, (nb, width)), 0.0)
                    for acc, one in zip(total, parts)
                ]
        for c in range(3):
            terms[k, i, c] = total[c]

    def send(k, f, t):
        if t == ttiles - 1:
            later_copy(k, f).start()
        if t == 0:
            earlier_copy(k, f).start()
        if f >= ftiles - REACH:
            up_copy(k, f, t).start()
        if f < REACH:
            down_copy(k, f, t).start()

    def arrived(k, t):
        for f in range(ftiles):
            if t == 0:
                later_copy(k, f).wait_recv()
            if t == ttiles - 1:
                earlier_copy(k, f).wait_recv()
        for f in range(ftiles - REACH, ftiles):
            up_copy(k, f, t).wait_recv()
        for f in range(REACH):
            down_copy(k, f, t).wait_recv()

    def update(k, t, change, scale):
        def at(f, t, c):
            if t < 0:
                return jnp.where(ti > 0, early[k, f, c], 0.0)
            if t >= ttiles:
                return jnp.where(ti < nt - 1, late[k, f, c], 0.0)
            if f < 0:
                return low[k, t * REACH + f + REACH, c]
            if f >= ftiles:
                return high[k, t * REACH + f - ftiles, c]
            return terms[k, at_tile(f, t), c]

        odd = lax.rem(k, 2) == 1
        for f in range(ftiles):
            i = at_tile(f, t)
            sums = [
                at(f, t, c)
                + coef[0] * (at(f - 1, t, c) + at(f + 1, t, c))
                + coef[1] * (at(f - 2, t, c) + at(f + 2, t, c))
                + coef[2] * (at(f, t - 1, c) + at(f, t + 1, c))
                for c in range(3)
            ]
            denom = sums[2] + coef[3]
            for c in range(2):
                old = gain[i, c]
                fresh = (sums[c] + prev[i, c]) / denom
                fresh = jnp.where(odd, 0.5 * (fresh + old), fresh)
                diff = fresh - old
                change = change + diff * diff
                scale = scale + fresh * fresh
                gain[i, c] = fresh
        return change, scale

    def record(k, change, scale):
        row = stats[...]
        for lane, value in ((k, change), (ITERS + k, scale)):
            total = jnp.sum(jnp.sum(value, axis=0, keepdims=True), axis=1, keepdims=True)
            row = jnp.where(lane_of == lane, total, row)
        stats[...] = row

    lane_of = lax.broadcasted_iota(jnp.int32, (1, width), 1)
    stats[...] = jnp.zeros_like(stats)
    zero = jnp.zeros((nb, width), F32)

    for f, t in tiles:
        for copy in loads(f, t):
            copy.wait()
        prepare(at_tile(f, t))
        tile_terms(0, f, t)
        if at_tile(f, t) == 0:
            pl.semaphore_wait(barrier, devices - 1)
            prior_copy.start()
        send(0, f, t)

    prior_copy.wait_recv()
    for f, t in tiles:
        i = at_tile(f, t)
        for c in range(2):
            if f == 0:
                for n in range(nb):
                    prev[i, c, n : n + 1, :] = from_prior[
                        t, c : c + 1, n * width : (n + 1) * width
                    ]
                prev[i, c] = prev[i, c] * coef[3]
            else:
                prev[i, c] = gain[at_tile(f - 1, t), c] * coef[3]

    def step(k, carry):
        change, scale = zero, zero
        for t in range(ttiles):
            arrived(k, t)
            change, scale = update(k, t, change, scale)
            for f in range(ftiles):
                tile_terms(k + 1, f, t)
                send(k + 1, f, t)
        record(k, change, scale)
        return carry

    lax.fori_loop(0, ITERS - 1, step, 0)
    change, scale = zero, zero
    for t in range(ttiles):
        arrived(ITERS - 1, t)
        change, scale = update(ITERS - 1, t, change, scale)
    record(ITERS - 1, change, scale)

    def stats_copy(step, row):
        return pltpu.make_async_remote_copy(
            src_ref=stats, dst_ref=all_stats.at[pl.ds(row, 1)],
            send_sem=stats_send.at[step], recv_sem=stats_recv.at[row],
            device_id=peer(step)[1], device_id_type=MESH,
        )

    def send_stats(step, carry):
        stats_copy(step, me).start()
        return carry

    lax.fori_loop(1, devices, send_stats, 0)
    all_stats[pl.ds(me, 1), :] = stats[...]

    for f, t in tiles:
        i = at_tile(f, t)
        for c in range(2):
            for n in range(nb):
                gains_ref[f, t, c : c + 1, n * width : (n + 1) * width] = gain[i, c, n : n + 1, :]

    def drain(k, carry):
        for f, t in tiles:
            if f >= ftiles - REACH:
                up_copy(k, f, t).wait_send()
            if f < REACH:
                down_copy(k, f, t).wait_send()
        for f in range(ftiles):
            later_copy(k, f).wait_send()
            earlier_copy(k, f).wait_send()
        return carry

    lax.fori_loop(0, ITERS, drain, 0)
    prior_copy.wait_send()

    def finish(step, carry):
        stats_copy(step, me).wait_send()
        stats_copy(step, peer(step)[0]).wait_recv()
        return carry

    lax.fori_loop(1, devices, finish, 0)
    whole = jnp.sum(all_stats[...], axis=0, keepdims=True)
    below_it = pltpu.roll(whole, width - ITERS, axis=1)
    changes_ref[...] = jnp.sqrt(whole / (below_it + 1e-06))


def hand_on(gains_in, changes_in, gains_ref, changes_ref):
    gains_ref[...] = gains_in[...]
    for k in range(ITERS):
        changes_ref[k] = changes_in[0, k]


def per_device(vis, model, block_rows, block_cols, flags, prior, couplings, damping):
    nf, nt = lax.axis_size("freq"), lax.axis_size("tm")
    ftiles, ttiles, blks = vis.shape[:3]
    width = vis.shape[-1]
    nb = prior.shape[-1] // width
    count = ftiles * ttiles
    dims = (nf, nt, ftiles, ttiles, blks, width, nb)
    vmem = pl.BlockSpec(memory_space=pltpu.VMEM)
    hbm = pl.BlockSpec(memory_space=pltpu.HBM)
    dma = pltpu.SemaphoreType.DMA
    halo = REACH * ttiles
    gains, changes = pl.pallas_call(
        functools.partial(kernel, dims),
        name="stefcal",
        out_shape=(
            jax.ShapeDtypeStruct(prior.shape, F32),
            jax.ShapeDtypeStruct((1, width), F32),
        ),
        in_specs=[hbm] * 8,
        out_specs=(vmem, vmem),
        scratch_shapes=[
            pltpu.SMEM(block_rows.shape, jnp.int32),
            pltpu.SMEM(block_rows.shape, jnp.int32),
            pltpu.SMEM(block_rows.shape, jnp.int32),
            pltpu.VMEM(prior.shape, F32),
            pltpu.VMEM(couplings.shape, F32),
            pltpu.VMEM((1, damping.shape[0]), F32),
            pltpu.VMEM((count,) + vis.shape[2:], BF16),
            pltpu.VMEM((count,) + vis.shape[2:], BF16),
            pltpu.VMEM((count * blks, 2 * width, 2 * width), BF16),
            pltpu.VMEM((count * blks // 2, 2 * width, 2 * width), BF16),
            pltpu.VMEM((count, 2, nb, width), F32),
            pltpu.VMEM((count, 2, nb, width), F32),
            pltpu.VMEM((4, nb, width), F32),
            pltpu.VMEM(prior.shape[1:], F32),
            pltpu.VMEM((ITERS, count, 3, nb, width), F32),
            pltpu.VMEM((ITERS, halo, 3, nb, width), F32),
            pltpu.VMEM((ITERS, halo, 3, nb, width), F32),
            pltpu.VMEM((ITERS, ftiles, 3, nb, width), F32),
            pltpu.VMEM((ITERS, ftiles, 3, nb, width), F32),
            pltpu.VMEM((1, width), F32),
            pltpu.VMEM((nf * nt, width), F32),
            dma((6,)),
            dma((2, count)),
            dma((2,)),
            dma((ITERS, halo)),
            dma((ITERS, halo)),
            dma((ITERS, halo)),
            dma((ITERS, halo)),
            dma((ITERS, ftiles)),
            dma((ITERS, ftiles)),
            dma((ITERS, ftiles)),
            dma((ITERS, ftiles)),
            dma((nf * nt,)),
            dma((nf * nt,)),
        ],
        compiler_params=pltpu.CompilerParams(
            collective_id=0, has_side_effects=True, vmem_limit_bytes=67043328
        ),
    )(vis, model, block_rows, block_cols, flags, prior, couplings, damping.reshape(1, -1))
    smem = pl.BlockSpec(memory_space=pltpu.SMEM)
    return pl.pallas_call(
        hand_on,
        name="hand_on",
        out_shape=(
            jax.ShapeDtypeStruct(prior.shape, F32),
            jax.ShapeDtypeStruct((ITERS,), F32),
        ),
        in_specs=[vmem, smem],
        out_specs=(vmem, smem),
    )(gains, changes)


def solution(mesh):
    placed = (
        P("freq", "tm", None, None, None, None),
        P("freq", "tm", None, None, None, None),
        P("freq", "tm", None),
        P("freq", "tm", None),
        P("freq", "tm", None),
        P("freq", "tm", None, None),
        P(),
        P(),
    )
    return jax.shard_map(
        per_device,
        mesh=mesh,
        in_specs=placed,
        out_specs=(P("freq", "tm", None, None), P()),
        check_vma=False,
    )
```

```python
import functools

import jax
import jax.numpy as jnp
from jax import lax
from jax.experimental import pallas as pl
from jax.experimental.pallas import tpu as pltpu
from jax.sharding import PartitionSpec as P

ITERS = 4
REACH = 2
MEET = 0
UNROLL = 8
MESH = pl.DeviceIdType.MESH
LOGICAL = pl.DeviceIdType.LOGICAL
F32 = jnp.float32
BF16 = jnp.bfloat16


def split(value):
    high = value.astype(BF16)
    return high, (value - high.astype(F32)).astype(BF16)


def kernel(
    dims,
    vis_ref, model_ref, rows_in, cols_in, flags_in, prior_in, coup_in, damp_in,
    gains_ref, all_stats_ref,
    rows_ref, cols_ref, flags_ref, prior_ref, coup_ref, damp_ref,
    data, wa, wb, gain, prev, coef, from_prior, terms, halo, early, late,
    stats,
    small_sem, load_sem, prior_sem, halo_send, halo_recv,
    early_send, late_send, early_recv, late_recv, stats_send, stats_recv, out_sem,
):
    nf, nt, ftiles, ttiles, blks, width, nb = dims
    fi = lax.axis_index("freq")
    ti = lax.axis_index("tm")
    above, below = lax.rem(fi + 1, nf), lax.rem(fi + nf - 1, nf)
    tiles = [(f, t) for t in range(ttiles) for f in range(ftiles)]

    def at_tile(f, t):
        return t * ftiles + f

    devices = nf * nt
    me = fi * nt + ti

    def peer(step):
        return lax.rem(me + step, devices)

    def loads(f, t):
        i = at_tile(f, t)
        return (
            pltpu.make_async_copy(vis_ref.at[f, t], data.at[i, 0], load_sem.at[i]),
            pltpu.make_async_copy(model_ref.at[f, t], data.at[i, 1], load_sem.at[i]),
        )

    for copy in loads(*tiles[0]):
        copy.start()
    small = [
        pltpu.make_async_copy(src, dst, small_sem.at[n])
        for n, (src, dst) in enumerate((
            (prior_in, prior_ref), (coup_in, coup_ref), (damp_in, damp_ref),
            (rows_in, rows_ref), (cols_in, cols_ref), (flags_in, flags_ref),
        ))
    ]
    for copy in small:
        copy.start()
    for f, t in tiles[1:]:
        for copy in loads(f, t):
            copy.start()

    barrier = pltpu.get_barrier_semaphore()

    def greet(step, carry):
        pl.semaphore_signal(barrier, inc=1, device_id=peer(step), device_id_type=LOGICAL)
        return carry

    lax.fori_loop(1, devices, greet, 0, unroll=UNROLL)

    def set_up():
        for f, t in tiles:
            i = at_tile(f, t)
            for c in range(2):
                for n in range(nb):
                    gain[i, c, n : n + 1, :] = prior_ref[f, t, c : c + 1, n * width : (n + 1) * width]
        for n in range(nb):
            for c in range(3):
                coef[c, n : n + 1, :] = coup_ref[c : c + 1, n * width : (n + 1) * width]
            coef[3, n : n + 1, :] = damp_ref[0:1, n * width : (n + 1) * width]

    prior_copy = pltpu.make_async_remote_copy(
        src_ref=prior_ref.at[ftiles - 1], dst_ref=from_prior,
        send_sem=prior_sem.at[0], recv_sem=prior_sem.at[1],
        device_id={"freq": above}, device_id_type=MESH,
    )

    def up_copy(k, f, t):
        return pltpu.make_async_remote_copy(
            src_ref=terms.at[k, at_tile(f, t)], dst_ref=halo.at[k, t, f - (ftiles - REACH)],
            send_sem=halo_send.at[0], recv_sem=halo_recv.at[k, t],
            device_id={"freq": above}, device_id_type=MESH,
        )

    def down_copy(k, f, t):
        return pltpu.make_async_remote_copy(
            src_ref=terms.at[k, at_tile(f, t)], dst_ref=halo.at[k, t, REACH + f],
            send_sem=halo_send.at[0], recv_sem=halo_recv.at[k, t],
            device_id={"freq": below}, device_id_type=MESH,
        )

    def later_copy(k, f):
        return pltpu.make_async_remote_copy(
            src_ref=terms.at[k, at_tile(f, ttiles - 1)], dst_ref=early.at[k, f],
            send_sem=early_send.at[0], recv_sem=early_recv.at[k],
            device_id={"tm": lax.rem(ti + 1, nt)}, device_id_type=MESH,
        )

    def earlier_copy(k, f):
        return pltpu.make_async_remote_copy(
            src_ref=terms.at[k, at_tile(f, 0)], dst_ref=late.at[k, f],
            send_sem=late_send.at[0], recv_sem=late_recv.at[k],
            device_id={"tm": lax.rem(ti + nt - 1, nt)}, device_id_type=MESH,
        )

    def wait_for(ref, sem):
        pltpu.make_async_copy(ref, ref, sem).wait()

    def prepare(i, p):
        for side in range(2):
            b = 2 * p + side
            lo = side * width
            v_re = data[i, 0, b, 0].astype(F32)
            v_im = data[i, 0, b, 1].astype(F32)
            m_re = data[i, 1, b, 0].astype(F32)
            m_im = data[i, 1, b, 1].astype(F32)
            re_hi, re_lo = split(v_re * m_re + v_im * m_im)
            im_hi, im_lo = split(v_re * m_im - v_im * m_re)
            sq_hi, sq_lo = split(m_re * m_re + m_im * m_im)
            wa[i * blks + b, 0:width, 0:width] = re_hi
            wa[i * blks + b, width:, 0:width] = im_hi
            wa[i * blks + b, 0:width, width:] = sq_hi
            wa[i * blks + b, width:, width:] = sq_lo
            wb[i * (blks // 2) + p, 0:width, lo : lo + width] = re_lo
            wb[i * (blks // 2) + p, width:, lo : lo + width] = im_lo

    row_of = lax.broadcasted_iota(jnp.int32, (8, width), 0)
    block_of = lax.broadcasted_iota(jnp.int32, (nb, width), 0)
    zero = jnp.zeros((nb, width), F32)

    def pair_terms(f, t, p, total):
        i = at_tile(f, t)
        highs, outs, cols = [], [], []
        for b in (2 * p, 2 * p + 1):
            row = rows_ref[f, t, b]
            cols.append(jnp.where(flags_ref[f, t, b] != 0, cols_ref[f, t, b], -1))
            re = jnp.broadcast_to(gain[i, 0, pl.ds(row, 1), :], (8, width))
            im = jnp.broadcast_to(gain[i, 1, pl.ds(row, 1), :], (8, width))
            sq = re * re + im * im
            left = jnp.where(row_of == 0, re, jnp.where(row_of == 1, im, sq))
            right = jnp.where(row_of == 0, -im, jnp.where(row_of == 1, re, sq))
            lhs = jnp.concatenate([left, right], axis=1)
            lhs_hi = lhs.astype(BF16).astype(F32)
            highs.append(lhs_hi)
            lhs = jnp.concatenate([lhs_hi, lhs - lhs_hi], axis=0).astype(BF16)
            out = jnp.dot(lhs, wa[i * blks + b], preferred_element_type=F32)
            outs.append(out[0:8] + out[8:16])
        low_out = jnp.dot(
            jnp.concatenate(highs, axis=0).astype(BF16),
            wb[i * (blks // 2) + p],
            preferred_element_type=F32,
        )
        low_outs = (low_out[0:8, 0:width], low_out[8:16, width:])
        for out, low_out, col in zip(outs, low_outs, cols):
            num = out[:, 0:width] + low_out
            den = out[:, width:]
            hit = block_of == col
            parts = (num[0:1], num[1:2], den[2:3])
            total = [
                acc + jnp.where(hit, jnp.broadcast_to(one, (nb, width)), 0.0)
                for acc, one in zip(total, parts)
            ]
        return total

    def keep(k, f, t, total):
        for c in range(3):
            terms[k, at_tile(f, t), c] = total[c]

    def tile_terms(k, f, t):
        total = [zero] * 3
        for p in range(blks // 2):
            total = pair_terms(f, t, p, total)
        keep(k, f, t, total)

    def send(k, f, t):
        if t == ttiles - 1:
            pl.when(ti < nt - 1)(later_copy(k, f).start)
        if t == 0:
            pl.when(ti > 0)(earlier_copy(k, f).start)
        if f >= ftiles - REACH:
            up_copy(k, f, t).start()
        if f < REACH:
            down_copy(k, f, t).start()

    def arrived(k, t):
        if t == 0:
            pl.when(ti > 0)(lambda: wait_for(early.at[k], early_recv.at[k]))
        if t == ttiles - 1:
            pl.when(ti < nt - 1)(lambda: wait_for(late.at[k], late_recv.at[k]))
        wait_for(halo.at[k, t], halo_recv.at[k, t])

    def update(k, t, change, scale):
        def at(f, t, c):
            if t < 0:
                return jnp.where(ti > 0, early[k, f, c], 0.0)
            if t >= ttiles:
                return jnp.where(ti < nt - 1, late[k, f, c], 0.0)
            if f < 0:
                return halo[k, t, f + REACH, c]
            if f >= ftiles:
                return halo[k, t, f - ftiles + REACH, c]
            return terms[k, at_tile(f, t), c]

        odd = lax.rem(k, 2) == 1
        for f in range(ftiles):
            i = at_tile(f, t)
            sums = [
                at(f, t, c)
                + coef[0] * (at(f - 1, t, c) + at(f + 1, t, c))
                + coef[1] * (at(f - 2, t, c) + at(f + 2, t, c))
                + coef[2] * (at(f, t - 1, c) + at(f, t + 1, c))
                for c in range(3)
            ]
            denom = sums[2] + coef[3]
            for c in range(2):
                old = gain[i, c]
                fresh = (sums[c] + prev[i, c]) / denom
                fresh = jnp.where(odd, 0.5 * (fresh + old), fresh)
                diff = fresh - old
                change = change + diff * diff
                scale = scale + fresh * fresh
                gain[i, c] = fresh
        return change, scale

    def record(k, change, scale):
        row = stats[...]
        for lane, value in ((k, change), (ITERS + k, scale)):
            total = jnp.sum(jnp.sum(value, axis=0, keepdims=True), axis=1, keepdims=True)
            row = jnp.where(lane_of == lane, total, row)
        stats[...] = row

    lane_of = lax.broadcasted_iota(jnp.int32, (1, width), 1)
    stats[...] = jnp.zeros_like(stats)
    def fetched(f, t):
        i = at_tile(f, t)
        pltpu.make_async_copy(data.at[i], data.at[i], load_sem.at[i]).wait()

    fetched(*tiles[0])

    def first_pair(p, carry):
        prepare(0, p)
        return carry

    def first_stage(n, f, t):
        total = [zero] * 3
        for p in range(blks // 2):
            total = pair_terms(f, t, p, total)
            prepare(n + 1, p)
        keep(0, f, t, total)

    lax.fori_loop(0, blks // 2, first_pair, 0)
    for copy in small:
        copy.wait()
    set_up()
    for n, (f, t) in enumerate(tiles):
        if n + 1 < len(tiles):
            fetched(*tiles[n + 1])

            first_stage(n, f, t)
        else:
            tile_terms(0, f, t)
        if n == MEET:
            pl.semaphore_wait(barrier, devices - 1)
            prior_copy.start()
        if n >= MEET:
            for f, t in tiles[(0 if n == MEET else n) : n + 1]:
                send(0, f, t)

    prior_copy.wait_recv()
    for f, t in tiles:
        i = at_tile(f, t)
        for c in range(2):
            if f == 0:
                for n in range(nb):
                    prev[i, c, n : n + 1, :] = from_prior[
                        t, c : c + 1, n * width : (n + 1) * width
                    ]
                prev[i, c] = prev[i, c] * coef[3]
            else:
                prev[i, c] = gain[at_tile(f - 1, t), c] * coef[3]

    def step(k, carry):
        change, scale = zero, zero
        for t in range(ttiles):
            arrived(k, t)
            change, scale = update(k, t, change, scale)
            for f in range(ftiles):
                tile_terms(k + 1, f, t)
                send(k + 1, f, t)
        record(k, change, scale)
        return carry

    lax.fori_loop(0, ITERS - 1, step, 0)
    change, scale = zero, zero
    for t in range(ttiles):
        arrived(ITERS - 1, t)
        change, scale = update(ITERS - 1, t, change, scale)
    record(ITERS - 1, change, scale)

    def stats_copy(step, row):
        return pltpu.make_async_remote_copy(
            src_ref=stats, dst_ref=all_stats_ref.at[row],
            send_sem=stats_send.at[0], recv_sem=stats_recv.at[0],
            device_id=peer(step), device_id_type=LOGICAL,
        )

    def send_stats(step, carry):
        stats_copy(step, me).start()
        return carry

    lax.fori_loop(1, devices, send_stats, 0, unroll=UNROLL)
    own_stats = pltpu.make_async_copy(stats, all_stats_ref.at[me], out_sem.at[1])
    own_stats.start()
    prior_copy.wait_send()
    for f, t in tiles:
        i = at_tile(f, t)
        for c in range(2):
            for n in range(nb):
                prior_ref[f, t, c : c + 1, n * width : (n + 1) * width] = gain[i, c, n : n + 1, :]
    gains_out = pltpu.make_async_copy(prior_ref, gains_ref, out_sem.at[0])
    gains_out.start()

    wait_for(halo, halo_send.at[0])
    pl.when(ti < nt - 1)(lambda: wait_for(early, early_send.at[0]))
    pl.when(ti > 0)(lambda: wait_for(late, late_send.at[0]))
    own_stats.wait()
    gains_out.wait()
    others = all_stats_ref.at[pl.ds(0, devices - 1)]
    wait_for(others, stats_send.at[0])
    wait_for(others, stats_recv.at[0])


def hand_on(gains_in, stats_in, gains_ref, changes_ref):
    gains_ref[...] = gains_in[...]
    whole = jnp.sum(stats_in[...], axis=0)
    scale = pltpu.roll(whole, whole.shape[1] - ITERS, axis=1)
    changes_ref[...] = jnp.sqrt(whole / (scale + 1e-06))[0, :ITERS]


def per_device(vis, model, block_rows, block_cols, flags, prior, couplings, damping):
    nf, nt = lax.axis_size("freq"), lax.axis_size("tm")
    ftiles, ttiles, blks = vis.shape[:3]
    width = vis.shape[-1]
    nb = prior.shape[-1] // width
    count = ftiles * ttiles
    dims = (nf, nt, ftiles, ttiles, blks, width, nb)
    vmem = pl.BlockSpec(memory_space=pltpu.VMEM)
    hbm = pl.BlockSpec(memory_space=pltpu.HBM)
    dma = pltpu.SemaphoreType.DMA
    gains, all_stats = pl.pallas_call(
        functools.partial(kernel, dims),
        name="stefcal",
        out_shape=(
            jax.ShapeDtypeStruct(prior.shape, F32),
            jax.ShapeDtypeStruct((nf * nt, 1, width), F32),
        ),
        in_specs=[hbm] * 8,
        out_specs=(hbm, hbm),
        scratch_shapes=[
            pltpu.SMEM(block_rows.shape, jnp.int32),
            pltpu.SMEM(block_rows.shape, jnp.int32),
            pltpu.SMEM(block_rows.shape, jnp.int32),
            pltpu.VMEM(prior.shape, F32),
            pltpu.VMEM(couplings.shape, F32),
            pltpu.VMEM((1, damping.shape[0]), F32),
            pltpu.VMEM((count, 2) + vis.shape[2:], BF16),
            pltpu.VMEM((count * blks, 2 * width, 2 * width), BF16),
            pltpu.VMEM((count * blks // 2, 2 * width, 2 * width), BF16),
            pltpu.VMEM((count, 2, nb, width), F32),
            pltpu.VMEM((count, 2, nb, width), F32),
            pltpu.VMEM((4, nb, width), F32),
            pltpu.VMEM(prior.shape[1:], F32),
            pltpu.VMEM((ITERS, count, 3, nb, width), F32),
            pltpu.VMEM((ITERS, ttiles, 2 * REACH, 3, nb, width), F32),
            pltpu.VMEM((ITERS, ftiles, 3, nb, width), F32),
            pltpu.VMEM((ITERS, ftiles, 3, nb, width), F32),
            pltpu.VMEM((1, width), F32),
            dma((6,)),
            dma((count,)),
            dma((2,)),
            dma((1,)),
            dma((ITERS, ttiles)),
            dma((1,)),
            dma((1,)),
            dma((ITERS,)),
            dma((ITERS,)),
            dma((1,)),
            dma((1,)),
            dma((2,)),
        ],
        compiler_params=pltpu.CompilerParams(
            collective_id=0, has_side_effects=True, vmem_limit_bytes=67043328
        ),
    )(vis, model, block_rows, block_cols, flags, prior, couplings, damping.reshape(1, -1))
    return pl.pallas_call(
        hand_on,
        name="hand_on",
        out_shape=(
            jax.ShapeDtypeStruct(prior.shape, F32),
            jax.ShapeDtypeStruct((ITERS,), F32),
        ),
        in_specs=[vmem, vmem],
        out_specs=(vmem, vmem),
    )(gains, all_stats)


def solution(mesh):
    placed = (
        P("freq", "tm", None, None, None, None),
        P("freq", "tm", None, None, None, None),
        P("freq", "tm", None),
        P("freq", "tm", None),
        P("freq", "tm", None),
        P("freq", "tm", None, None),
        P(),
        P(),
    )
    return jax.shard_map(
        per_device,
        mesh=mesh,
        in_specs=placed,
        out_specs=(P("freq", "tm", None, None), P()),
        check_vma=False,
    )
```

```python
import functools

import jax
import jax.numpy as jnp
from jax import lax
from jax.experimental import pallas as pl
from jax.experimental.pallas import tpu as pltpu
from jax.sharding import PartitionSpec as P

ITERS = 4
REACH = 2
EARLY = 2
UNROLL = 8
CHUNK = 16
VPU_PART = (0, 16)
PARTS = 4
MESH = pl.DeviceIdType.MESH
LOGICAL = pl.DeviceIdType.LOGICAL
F32 = jnp.float32
BF16 = jnp.bfloat16


def split(value):
    high = value.astype(BF16)
    return high, (value - high.astype(F32)).astype(BF16)


def kernel(
    dims,
    vis_ref, model_ref, rows_in, cols_in, flags_in, prior_in, coup_in, damp_in,
    gains_ref, all_stats_ref,
    rows_ref, cols_ref, flags_ref, prior_ref, coup_ref, damp_ref,
    data, wa, wb, cv, gain, prev, coef, from_prior, terms, halo, early, late,
    stats,
    small_sem, load_sem, prior_sem, halo_send, halo_recv,
    early_send, late_send, early_recv, late_recv, stats_send, stats_recv, out_sem,
):
    nf, nt, ftiles, ttiles, blks, width, nb, on_mxu = dims
    on_vpu = blks - on_mxu
    fi = lax.axis_index("freq")
    ti = lax.axis_index("tm")
    above, below = lax.rem(fi + 1, nf), lax.rem(fi + nf - 1, nf)
    order = range(ftiles - 1, -1, -1)
    tiles = [(f, t) for t in range(ttiles) for f in order]

    def at_tile(f, t):
        return t * ftiles + f

    devices = nf * nt
    me = fi * nt + ti

    def peer(step):
        return lax.rem(me + step, devices)

    def load(f, t, part):
        i, size = at_tile(f, t), blks // PARTS
        some = pl.ds(part * size, size)
        for n, ref in enumerate((vis_ref, model_ref)):
            pltpu.make_async_copy(
                ref.at[f, t, some], data.at[i, n, some], load_sem.at[i, part]
            ).start()

    def loaded(f, t, part):
        i, size = at_tile(f, t), blks // PARTS
        some = pl.ds(part * size, size)
        wait_for(data.at[i, :, some], load_sem.at[i, part])

    def wait_for(ref, sem):
        pltpu.make_async_copy(ref, ref, sem).wait()

    small = [
        pltpu.make_async_copy(src, dst, small_sem.at[n])
        for n, (src, dst) in enumerate((
            (prior_in, prior_ref), (coup_in, coup_ref), (damp_in, damp_ref),
            (rows_in, rows_ref), (cols_in, cols_ref), (flags_in, flags_ref),
        ))
    ]
    for copy in small:
        copy.start()
    for f, t in tiles[:2]:
        for part in range(PARTS):
            load(f, t, part)

    barrier = pltpu.get_barrier_semaphore()

    def greet(step, carry):
        pl.semaphore_signal(barrier, inc=1, device_id=peer(step), device_id_type=LOGICAL)
        return carry

    lax.fori_loop(1, devices, greet, 0, unroll=UNROLL)

    def set_up():
        for f, t in tiles:
            i = at_tile(f, t)
            for c in range(2):
                for n in range(nb):
                    gain[i, c, n : n + 1, :] = prior_ref[f, t, c : c + 1, n * width : (n + 1) * width]
        for n in range(nb):
            for c in range(3):
                coef[c, n : n + 1, :] = coup_ref[c : c + 1, n * width : (n + 1) * width]
            coef[3, n : n + 1, :] = damp_ref[0:1, n * width : (n + 1) * width]

    prior_copy = pltpu.make_async_remote_copy(
        src_ref=prior_ref.at[ftiles - 1], dst_ref=from_prior,
        send_sem=prior_sem.at[0], recv_sem=prior_sem.at[1],
        device_id={"freq": above}, device_id_type=MESH,
    )

    def up_copy(k, f, t):
        return pltpu.make_async_remote_copy(
            src_ref=terms.at[k, at_tile(f, t)], dst_ref=halo.at[k, t, f - (ftiles - REACH)],
            send_sem=halo_send.at[0], recv_sem=halo_recv.at[k, t, int(f == ftiles - REACH)],
            device_id={"freq": above}, device_id_type=MESH,
        )

    def down_copy(k, f, t):
        return pltpu.make_async_remote_copy(
            src_ref=terms.at[k, at_tile(f, t)], dst_ref=halo.at[k, t, REACH + f],
            send_sem=halo_send.at[0], recv_sem=halo_recv.at[k, t, 0],
            device_id={"freq": below}, device_id_type=MESH,
        )

    def later_copy(k, f):
        return pltpu.make_async_remote_copy(
            src_ref=terms.at[k, at_tile(f, ttiles - 1)], dst_ref=early.at[k, f],
            send_sem=early_send.at[0], recv_sem=early_recv.at[k],
            device_id={"tm": lax.rem(ti + 1, nt)}, device_id_type=MESH,
        )

    def earlier_copy(k, f):
        return pltpu.make_async_remote_copy(
            src_ref=terms.at[k, at_tile(f, 0)], dst_ref=late.at[k, f],
            send_sem=late_send.at[0], recv_sem=late_recv.at[k],
            device_id={"tm": lax.rem(ti + nt - 1, nt)}, device_id_type=MESH,
        )

    def prepare(i, b, slot, side):
        for r in range(0, width, CHUNK):
            at = pl.ds(r, CHUNK)
            v_re = data[i, 0, b, 0, at].astype(F32)
            v_im = data[i, 0, b, 1, at].astype(F32)
            m_re = data[i, 1, b, 0, at].astype(F32)
            m_im = data[i, 1, b, 1, at].astype(F32)
            re = v_re * m_re + v_im * m_im
            im = v_re * m_im - v_im * m_re
            sq = m_re * m_re + m_im * m_im
            if side is None:
                for c, value in enumerate((re, im, sq)):
                    cv[i, slot, c, at] = value
                continue
            lower = pl.ds(width + r, CHUNK)
            wa[i, 2 * slot + side, 0, at], wb[i, slot, side, at] = split(re)
            wa[i, 2 * slot + side, 0, lower], wb[i, slot, side, lower] = split(im)
            wa[i, 2 * slot + side, 1, at], wa[i, 2 * slot + side, 1, lower] = split(sq)

    def prepare_pair(i, p):
        for side in range(2):
            prepare(i, 2 * p + side, p, side)

    def prepare_tile(i, part):
        def pair(p, carry):
            prepare_pair(i, p)
            return carry

        size = blks // 2 // PARTS
        lax.fori_loop(part * size, part * size + size, pair, 0)

    row_of = lax.broadcasted_iota(jnp.int32, (8, width), 0)
    block_of = lax.broadcasted_iota(jnp.int32, (nb, width), 0)
    zero = jnp.zeros((nb, width), F32)

    def column(f, t, b):
        return jnp.where(flags_ref[f, t, b] != 0, cols_ref[f, t, b], -1)

    def gains_of(f, t, b):
        row, i = rows_ref[f, t, b], at_tile(f, t)
        return gain[i, 0, pl.ds(row, 1), :], gain[i, 1, pl.ds(row, 1), :]

    def add(total, col, parts):
        hit = block_of == col
        return [
            acc + jnp.where(hit, jnp.broadcast_to(one, (nb, width)), 0.0)
            for acc, one in zip(total, parts)
        ]

    def pair_terms(f, t, p, total):
        i = at_tile(f, t)
        highs, outs, cols = [], [], []
        for side in range(2):
            b = 2 * p + side
            cols.append(column(f, t, b))
            re, im = (jnp.broadcast_to(x, (8, width)) for x in gains_of(f, t, b))
            sq = re * re + im * im
            left = jnp.where(row_of == 0, re, jnp.where(row_of == 1, im, sq))
            right = jnp.where(row_of == 0, -im, jnp.where(row_of == 1, re, sq))
            lhs = jnp.concatenate([left, right], axis=1)
            lhs_hi = lhs.astype(BF16).astype(F32)
            highs.append(lhs_hi)
            lhs = jnp.concatenate([lhs_hi, lhs - lhs_hi], axis=0).astype(BF16)
            rhs = jnp.concatenate([wa[i, b, 0], wa[i, b, 1]], axis=1)
            out = jnp.dot(lhs, rhs, preferred_element_type=F32)
            outs.append(out[0:8] + out[8:16])
        low_out = jnp.dot(
            jnp.concatenate(highs, axis=0).astype(BF16),
            jnp.concatenate([wb[i, p, 0], wb[i, p, 1]], axis=1),
            preferred_element_type=F32,
        )
        low_outs = (low_out[0:8, 0:width], low_out[8:16, width:])
        for out, low_out, col in zip(outs, low_outs, cols):
            num = out[:, 0:width] + low_out
            total = add(total, col, (num[0:1], num[1:2], out[2:3, width:]))
        return total

    def spread(f, t):
        rows = [gains_of(f, t, on_mxu + v) for v in range(on_vpu)]
        pad = [jnp.zeros((-on_vpu % 8, width), F32)] if on_vpu % 8 else []
        re, im = (jnp.concatenate([x[c] for x in rows] + pad, axis=0) for c in range(2))
        return jnp.concatenate([re, im, re * re + im * im], axis=0).T, re.shape[0]

    def plain_terms(f, t, v, turned, total):
        across, apart = turned
        i = at_tile(f, t)
        sums = [jnp.zeros((8, width), F32)] * 3
        for r in range(0, width, 8):
            g_re, g_im, g_sq = (
                jnp.broadcast_to(
                    across[r : r + 8, c * apart + v : c * apart + v + 1], (8, width)
                )
                for c in range(3)
            )
            re, im, sq = (cv[i, v, c, r : r + 8] for c in range(3))
            sums[0] = sums[0] + (re * g_re - im * g_im)
            sums[1] = sums[1] + (im * g_re + re * g_im)
            sums[2] = sums[2] + sq * g_sq
        parts = [jnp.sum(x, axis=0, keepdims=True) for x in sums]
        return add(total, column(f, t, on_mxu + v), parts)

    def keep(k, f, t, total):
        for c in range(3):
            terms[k, at_tile(f, t), c] = total[c]

    def tile_terms(k, f, t):
        total = [zero] * 3
        turned = spread(f, t) if on_vpu else None
        for n in range(max(on_mxu // 2, on_vpu)):
            if n < on_mxu // 2:
                total = pair_terms(f, t, n, total)
            if n < on_vpu:
                total = plain_terms(f, t, n, turned, total)
        keep(k, f, t, total)

    def first_stage(n, f, t):
        for part in range(PARTS):
            prepare_tile(at_tile(*tiles[n + 1]), part)
        tile_terms(0, f, t)

    outer = lax.rem(fi, 2) == 1

    def send_up(k, f, t):
        if f >= ftiles - REACH:
            up_copy(k, f, t).start()

    def send_down(k, f, t):
        if f < REACH:
            down_copy(k, f, t).start()

    def send(k, f, t):
        if t == ttiles - 1:
            pl.when(ti < nt - 1)(later_copy(k, f).start)
        if t == 0:
            pl.when(ti > 0)(earlier_copy(k, f).start)
        pl.when(outer)(lambda: send_up(k, f, t))
        pl.when(jnp.logical_not(outer))(lambda: send_down(k, f, t))

    def send_rest(k, f, t):
        pl.when(outer)(lambda: send_down(k, f, t))
        pl.when(jnp.logical_not(outer))(lambda: send_up(k, f, t))

    def arrived(k, f, t):
        if f == ftiles - 1:
            if t == 0:
                pl.when(ti > 0)(lambda: wait_for(early.at[k], early_recv.at[k]))
            if t == ttiles - 1:
                pl.when(ti < nt - 1)(lambda: wait_for(late.at[k], late_recv.at[k]))
            wait_for(halo.at[k, t, pl.ds(1, 2 * REACH - 1)], halo_recv.at[k, t, 0])
        if f == 0:
            wait_for(halo.at[k, t, 0], halo_recv.at[k, t, 1])

    def update(k, f, t, change, scale):
        def at(f, t, c):
            if t < 0:
                return jnp.where(ti > 0, early[k, f, c], 0.0)
            if t >= ttiles:
                return jnp.where(ti < nt - 1, late[k, f, c], 0.0)
            if f < 0:
                return halo[k, t, f + REACH, c]
            if f >= ftiles:
                return halo[k, t, f - ftiles + REACH, c]
            return terms[k, at_tile(f, t), c]

        odd = lax.rem(k, 2) == 1
        i = at_tile(f, t)
        sums = [
            at(f, t, c)
            + coef[0] * (at(f - 1, t, c) + at(f + 1, t, c))
            + coef[1] * (at(f - 2, t, c) + at(f + 2, t, c))
            + coef[2] * (at(f, t - 1, c) + at(f, t + 1, c))
            for c in range(3)
        ]
        denom = sums[2] + coef[3]
        for c in range(2):
            old = gain[i, c]
            fresh = (sums[c] + prev[i, c]) / denom
            fresh = jnp.where(odd, 0.5 * (fresh + old), fresh)
            diff = fresh - old
            change = change + diff * diff
            scale = scale + fresh * fresh
            gain[i, c] = fresh
        return change, scale

    def record(k, change, scale):
        row = stats[...]
        for lane, value in ((k, change), (ITERS + k, scale)):
            total = jnp.sum(jnp.sum(value, axis=0, keepdims=True), axis=1, keepdims=True)
            row = jnp.where(lane_of == lane, total, row)
        stats[...] = row

    lane_of = lax.broadcasted_iota(jnp.int32, (1, width), 1)
    stats[...] = jnp.zeros_like(stats)
    for part in range(PARTS):
        loaded(*tiles[0], part)
        if len(tiles) > 2:
            load(*tiles[2], part)
        prepare_tile(at_tile(*tiles[0]), part)
    for copy in small:
        copy.wait()
    set_up()
    last = len(tiles) - 1
    ahead = me < EARLY

    def meet(n, ready):
        def go():
            pl.semaphore_wait(barrier, devices - 1)

        def pass_on(some):
            for f, t in some:
                send(0, f, t)
                send_rest(0, f, t)

        @pl.when(jnp.logical_not(ahead))
        def _():
            if n == 0:
                go()
            pass_on(ready)
            if n == 0:
                prior_copy.start()

        if n == last:
            @pl.when(ahead)
            def _():
                go()
                pass_on(tiles)
                prior_copy.start()

    for n, (f, t) in enumerate(tiles):
        if n + 1 < len(tiles):
            for part in range(PARTS):
                loaded(*tiles[n + 1], part)
                if n + 3 < len(tiles):
                    load(*tiles[n + 3], part)
            first_stage(n, f, t)
        else:
            tile_terms(0, f, t)
        meet(n, [(f, t)])

    for f, t in tiles:
        if f > 0:
            for c in range(2):
                prev[at_tile(f, t), c] = gain[at_tile(f - 1, t), c] * coef[3]

    def take_prior():
        prior_copy.wait_recv()
        for t in range(ttiles):
            i = at_tile(0, t)
            for c in range(2):
                for n in range(nb):
                    prev[i, c, n : n + 1, :] = from_prior[
                        t, c : c + 1, n * width : (n + 1) * width
                    ]
                prev[i, c] = prev[i, c] * coef[3]

    def step(k, carry):
        change, scale = zero, zero
        for f, t in tiles:
            arrived(k, f, t)
            if f == 0 and t == 0:
                pl.when(k == 0)(take_prior)
            change, scale = update(k, f, t, change, scale)
            tile_terms(k + 1, f, t)
            send(k + 1, f, t)
            send_rest(k + 1, f, t)
        record(k, change, scale)
        return carry

    lax.fori_loop(0, ITERS - 1, step, 0)
    change, scale = zero, zero
    for f, t in tiles:
        arrived(ITERS - 1, f, t)
        change, scale = update(ITERS - 1, f, t, change, scale)
    record(ITERS - 1, change, scale)

    def stats_copy(step, row):
        return pltpu.make_async_remote_copy(
            src_ref=stats, dst_ref=all_stats_ref.at[row],
            send_sem=stats_send.at[0], recv_sem=stats_recv.at[0],
            device_id=peer(step), device_id_type=LOGICAL,
        )

    def send_stats(step, carry):
        stats_copy(step, me).start()
        return carry

    lax.fori_loop(1, devices, send_stats, 0, unroll=UNROLL)
    own_stats = pltpu.make_async_copy(stats, all_stats_ref.at[me], out_sem.at[1])
    own_stats.start()
    prior_copy.wait_send()
    for f, t in tiles:
        i = at_tile(f, t)
        for c in range(2):
            for n in range(nb):
                prior_ref[f, t, c : c + 1, n * width : (n + 1) * width] = gain[i, c, n : n + 1, :]
    gains_out = pltpu.make_async_copy(prior_ref, gains_ref, out_sem.at[0])
    gains_out.start()

    wait_for(halo, halo_send.at[0])
    pl.when(ti < nt - 1)(lambda: wait_for(early, early_send.at[0]))
    pl.when(ti > 0)(lambda: wait_for(late, late_send.at[0]))
    own_stats.wait()
    gains_out.wait()
    others = all_stats_ref.at[pl.ds(0, devices - 1)]
    wait_for(others, stats_send.at[0])
    wait_for(others, stats_recv.at[0])


def hand_on(gains_in, stats_in, gains_ref, changes_ref):
    gains_ref[...] = gains_in[...]
    whole = jnp.sum(stats_in[...], axis=0)
    scale = pltpu.roll(whole, whole.shape[1] - ITERS, axis=1)
    changes_ref[...] = jnp.sqrt(whole / (scale + 1e-06))[0, :ITERS]


def per_device(vis, model, block_rows, block_cols, flags, prior, couplings, damping):
    nf, nt = lax.axis_size("freq"), lax.axis_size("tm")
    ftiles, ttiles, blks = vis.shape[:3]
    width = vis.shape[-1]
    nb = prior.shape[-1] // width
    count = ftiles * ttiles
    on_vpu = VPU_PART[0] * blks // VPU_PART[1]
    on_mxu = blks - on_vpu
    assert on_mxu % 2 == 0
    dims = (nf, nt, ftiles, ttiles, blks, width, nb, on_mxu)
    vmem = pl.BlockSpec(memory_space=pltpu.VMEM)
    hbm = pl.BlockSpec(memory_space=pltpu.HBM)
    dma = pltpu.SemaphoreType.DMA
    gains, all_stats = pl.pallas_call(
        functools.partial(kernel, dims),
        name="stefcal",
        out_shape=(
            jax.ShapeDtypeStruct(prior.shape, F32),
            jax.ShapeDtypeStruct((nf * nt, 1, width), F32),
        ),
        in_specs=[hbm] * 8,
        out_specs=(hbm, hbm),
        scratch_shapes=[
            pltpu.SMEM(block_rows.shape, jnp.int32),
            pltpu.SMEM(block_rows.shape, jnp.int32),
            pltpu.SMEM(block_rows.shape, jnp.int32),
            pltpu.VMEM(prior.shape, F32),
            pltpu.VMEM(couplings.shape, F32),
            pltpu.VMEM((1, damping.shape[0]), F32),
            pltpu.VMEM((count, 2) + vis.shape[2:], BF16),
            pltpu.VMEM((count, on_mxu, 2, 2 * width, width), BF16),
            pltpu.VMEM((count, on_mxu // 2, 2, 2 * width, width), BF16),
            pltpu.VMEM((count, max(on_vpu, 1), 3, width, width), F32),
            pltpu.VMEM((count, 2, nb, width), F32),
            pltpu.VMEM((count, 2, nb, width), F32),
            pltpu.VMEM((4, nb, width), F32),
            pltpu.VMEM(prior.shape[1:], F32),
            pltpu.VMEM((ITERS, count, 3, nb, width), F32),
            pltpu.VMEM((ITERS, ttiles, 2 * REACH, 3, nb, width), F32),
            pltpu.VMEM((ITERS, ftiles, 3, nb, width), F32),
            pltpu.VMEM((ITERS, ftiles, 3, nb, width), F32),
            pltpu.VMEM((1, width), F32),
            dma((6,)),
            dma((count, PARTS)),
            dma((2,)),
            dma((1,)),
            dma((ITERS, ttiles, 2)),
            dma((1,)),
            dma((1,)),
            dma((ITERS,)),
            dma((ITERS,)),
            dma((1,)),
            dma((1,)),
            dma((2,)),
        ],
        compiler_params=pltpu.CompilerParams(
            collective_id=0, has_side_effects=True, vmem_limit_bytes=67043328
        ),
    )(vis, model, block_rows, block_cols, flags, prior, couplings, damping.reshape(1, -1))
    return pl.pallas_call(
        hand_on,
        name="hand_on",
        out_shape=(
            jax.ShapeDtypeStruct(prior.shape, F32),
            jax.ShapeDtypeStruct((ITERS,), F32),
        ),
        in_specs=[vmem, vmem],
        out_specs=(vmem, vmem),
    )(gains, all_stats)


def solution(mesh):
    placed = (
        P("freq", "tm", None, None, None, None),
        P("freq", "tm", None, None, None, None),
        P("freq", "tm", None),
        P("freq", "tm", None),
        P("freq", "tm", None),
        P("freq", "tm", None, None),
        P(),
        P(),
    )
    return jax.shard_map(
        per_device,
        mesh=mesh,
        in_specs=placed,
        out_specs=(P("freq", "tm", None, None), P()),
        check_vma=False,
    )
```

```python
import functools

import jax
import jax.numpy as jnp
from jax import lax
from jax.experimental import pallas as pl
from jax.experimental.pallas import tpu as pltpu
from jax.sharding import PartitionSpec as P

ITERS = 4
REACH = 2
EARLY = 2
UNROLL = 8
CHUNK = 16
PARTS = 4
MESH = pl.DeviceIdType.MESH
LOGICAL = pl.DeviceIdType.LOGICAL
F32 = jnp.float32
BF16 = jnp.bfloat16


def split(value):
    high = value.astype(BF16)
    return high, (value - high.astype(F32)).astype(BF16)


def kernel(
    dims,
    vis_ref, model_ref, rows_in, cols_in, flags_in, prior_in, coup_in, damp_in,
    gains_ref, all_stats_ref,
    rows_ref, cols_ref, flags_ref, prior_ref, coup_ref, damp_ref,
    data, wa, wb, gain, prev, coef, from_prior, terms, halo, early, late,
    stats,
    small_sem, load_sem, prior_sem, halo_send, halo_recv,
    early_send, late_send, early_recv, late_recv, stats_send, stats_recv, out_sem,
):
    nf, nt, ftiles, ttiles, blks, width, nb = dims
    fi = lax.axis_index("freq")
    ti = lax.axis_index("tm")
    above, below = lax.rem(fi + 1, nf), lax.rem(fi + nf - 1, nf)
    order = range(ftiles - 1, -1, -1)
    tiles = [(f, t) for t in range(ttiles) for f in order]

    def at_tile(f, t):
        return t * ftiles + f

    devices = nf * nt
    me = fi * nt + ti

    def peer(step):
        return lax.rem(me + step, devices)

    def load(f, t, part):
        i, size = at_tile(f, t), blks // PARTS
        some = pl.ds(part * size, size)
        for n, ref in enumerate((vis_ref, model_ref)):
            pltpu.make_async_copy(
                ref.at[f, t, some], data.at[i, n, some], load_sem.at[i, part]
            ).start()

    def loaded(f, t, part):
        i, size = at_tile(f, t), blks // PARTS
        some = pl.ds(part * size, size)
        wait_for(data.at[i, :, some], load_sem.at[i, part])

    def wait_for(ref, sem):
        pltpu.make_async_copy(ref, ref, sem).wait()

    small = [
        pltpu.make_async_copy(src, dst, small_sem.at[n])
        for n, (src, dst) in enumerate((
            (prior_in, prior_ref), (coup_in, coup_ref), (damp_in, damp_ref),
            (rows_in, rows_ref), (cols_in, cols_ref), (flags_in, flags_ref),
        ))
    ]
    for copy in small:
        copy.start()
    for f, t in tiles[:2]:
        for part in range(PARTS):
            load(f, t, part)

    barrier = pltpu.get_barrier_semaphore()

    def greet(step, carry):
        pl.semaphore_signal(barrier, inc=1, device_id=peer(step), device_id_type=LOGICAL)
        return carry

    lax.fori_loop(1, devices, greet, 0, unroll=UNROLL)

    def set_up():
        for f, t in tiles:
            i = at_tile(f, t)
            for c in range(2):
                for n in range(nb):
                    gain[i, c, n : n + 1, :] = prior_ref[f, t, c : c + 1, n * width : (n + 1) * width]
        for n in range(nb):
            for c in range(3):
                coef[c, n : n + 1, :] = coup_ref[c : c + 1, n * width : (n + 1) * width]
            coef[3, n : n + 1, :] = damp_ref[0:1, n * width : (n + 1) * width]

    prior_copy = pltpu.make_async_remote_copy(
        src_ref=prior_ref.at[ftiles - 1], dst_ref=from_prior,
        send_sem=prior_sem.at[0], recv_sem=prior_sem.at[1],
        device_id={"freq": above}, device_id_type=MESH,
    )

    def up_copy(k, f, t):
        return pltpu.make_async_remote_copy(
            src_ref=terms.at[k, at_tile(f, t)], dst_ref=halo.at[k, t, f - (ftiles - REACH)],
            send_sem=halo_send.at[0], recv_sem=halo_recv.at[k, t, int(f == ftiles - REACH)],
            device_id={"freq": above}, device_id_type=MESH,
        )

    def down_copy(k, f, t):
        return pltpu.make_async_remote_copy(
            src_ref=terms.at[k, at_tile(f, t)], dst_ref=halo.at[k, t, REACH + f],
            send_sem=halo_send.at[0], recv_sem=halo_recv.at[k, t, 0],
            device_id={"freq": below}, device_id_type=MESH,
        )

    def later_copy(k, f):
        return pltpu.make_async_remote_copy(
            src_ref=terms.at[k, at_tile(f, ttiles - 1)], dst_ref=early.at[k, f],
            send_sem=early_send.at[0], recv_sem=early_recv.at[k],
            device_id={"tm": lax.rem(ti + 1, nt)}, device_id_type=MESH,
        )

    def earlier_copy(k, f):
        return pltpu.make_async_remote_copy(
            src_ref=terms.at[k, at_tile(f, 0)], dst_ref=late.at[k, f],
            send_sem=late_send.at[0], recv_sem=late_recv.at[k],
            device_id={"tm": lax.rem(ti + nt - 1, nt)}, device_id_type=MESH,
        )

    def prepare(i, b, slot, side):
        for r in range(0, width, CHUNK):
            at = pl.ds(r, CHUNK)
            v_re = data[i, 0, b, 0, at].astype(F32)
            v_im = data[i, 0, b, 1, at].astype(F32)
            m_re = data[i, 1, b, 0, at].astype(F32)
            m_im = data[i, 1, b, 1, at].astype(F32)
            re = v_re * m_re + v_im * m_im
            im = v_re * m_im - v_im * m_re
            sq = m_re * m_re + m_im * m_im
            lower = pl.ds(width + r, CHUNK)
            wa[i, 2 * slot + side, 0, at], wb[i, slot, side, at] = split(re)
            wa[i, 2 * slot + side, 0, lower], wb[i, slot, side, lower] = split(im)
            wa[i, 2 * slot + side, 1, at], wa[i, 2 * slot + side, 1, lower] = split(sq)

    def prepare_pair(i, p):
        for side in range(2):
            prepare(i, 2 * p + side, p, side)

    def prepare_tile(i, part):
        def pair(p, carry):
            prepare_pair(i, p)
            return carry

        size = blks // 2 // PARTS
        lax.fori_loop(part * size, part * size + size, pair, 0)

    row_of = lax.broadcasted_iota(jnp.int32, (8, width), 0)
    block_of = lax.broadcasted_iota(jnp.int32, (nb, width), 0)
    zero = jnp.zeros((nb, width), F32)

    def column(f, t, b):
        return jnp.where(flags_ref[f, t, b] != 0, cols_ref[f, t, b], -1)

    def gains_of(f, t, b):
        row, i = rows_ref[f, t, b], at_tile(f, t)
        return gain[i, 0, pl.ds(row, 1), :], gain[i, 1, pl.ds(row, 1), :]

    def add(total, col, parts):
        hit = block_of == col
        return [
            acc + jnp.where(hit, jnp.broadcast_to(one, (nb, width)), 0.0)
            for acc, one in zip(total, parts)
        ]

    def pair_terms(f, t, p, total):
        i = at_tile(f, t)
        highs, outs, cols = [], [], []
        for side in range(2):
            b = 2 * p + side
            cols.append(column(f, t, b))
            re, im = (jnp.broadcast_to(x, (8, width)) for x in gains_of(f, t, b))
            sq = re * re + im * im
            left = jnp.where(row_of == 0, re, jnp.where(row_of == 1, im, sq))
            right = jnp.where(row_of == 0, -im, jnp.where(row_of == 1, re, sq))
            lhs = jnp.concatenate([left, right], axis=1)
            lhs_hi = lhs.astype(BF16).astype(F32)
            highs.append(lhs_hi)
            lhs = jnp.concatenate([lhs_hi, lhs - lhs_hi], axis=0).astype(BF16)
            rhs = jnp.concatenate([wa[i, b, 0], wa[i, b, 1]], axis=1)
            out = jnp.dot(lhs, rhs, preferred_element_type=F32)
            outs.append(out[0:8] + out[8:16])
        low_out = jnp.dot(
            jnp.concatenate(highs, axis=0).astype(BF16),
            jnp.concatenate([wb[i, p, 0], wb[i, p, 1]], axis=1),
            preferred_element_type=F32,
        )
        low_outs = (low_out[0:8, 0:width], low_out[8:16, width:])
        for out, low_out, col in zip(outs, low_outs, cols):
            num = out[:, 0:width] + low_out
            total = add(total, col, (num[0:1], num[1:2], out[2:3, width:]))
        return total

    def keep(k, f, t, total):
        for c in range(3):
            terms[k, at_tile(f, t), c] = total[c]

    def tile_terms(k, f, t):
        total = [zero] * 3
        for p in range(blks // 2):
            total = pair_terms(f, t, p, total)
        keep(k, f, t, total)

    outer = lax.rem(fi, 2) == 1

    def send_up(k, f, t):
        if f >= ftiles - REACH:
            up_copy(k, f, t).start()

    def send_down(k, f, t):
        if f < REACH:
            down_copy(k, f, t).start()

    def send(k, f, t):
        if t == ttiles - 1:
            pl.when(ti < nt - 1)(later_copy(k, f).start)
        if t == 0:
            pl.when(ti > 0)(earlier_copy(k, f).start)
        pl.when(outer)(lambda: send_up(k, f, t))
        pl.when(jnp.logical_not(outer))(lambda: send_down(k, f, t))

    def send_rest(k, f, t):
        pl.when(outer)(lambda: send_down(k, f, t))
        pl.when(jnp.logical_not(outer))(lambda: send_up(k, f, t))

    def arrived(k, f, t):
        if f == ftiles - 1:
            if t == 0:
                pl.when(ti > 0)(lambda: wait_for(early.at[k], early_recv.at[k]))
            if t == ttiles - 1:
                pl.when(ti < nt - 1)(lambda: wait_for(late.at[k], late_recv.at[k]))
            wait_for(halo.at[k, t, pl.ds(1, 2 * REACH - 1)], halo_recv.at[k, t, 0])
        if f == 0:
            wait_for(halo.at[k, t, 0], halo_recv.at[k, t, 1])

    def update(k, f, t, change, scale):
        def at(f, t, c):
            if t < 0:
                return jnp.where(ti > 0, early[k, f, c], 0.0)
            if t >= ttiles:
                return jnp.where(ti < nt - 1, late[k, f, c], 0.0)
            if f < 0:
                return halo[k, t, f + REACH, c]
            if f >= ftiles:
                return halo[k, t, f - ftiles + REACH, c]
            return terms[k, at_tile(f, t), c]

        odd = lax.rem(k, 2) == 1
        i = at_tile(f, t)
        sums = [
            at(f, t, c)
            + coef[0] * (at(f - 1, t, c) + at(f + 1, t, c))
            + coef[1] * (at(f - 2, t, c) + at(f + 2, t, c))
            + coef[2] * (at(f, t - 1, c) + at(f, t + 1, c))
            for c in range(3)
        ]
        denom = sums[2] + coef[3]
        for c in range(2):
            old = gain[i, c]
            fresh = (sums[c] + prev[i, c]) / denom
            fresh = jnp.where(odd, 0.5 * (fresh + old), fresh)
            diff = fresh - old
            change = change + diff * diff
            scale = scale + fresh * fresh
            gain[i, c] = fresh
        return change, scale

    def record(k, change, scale):
        row = stats[...]
        for lane, value in ((k, change), (ITERS + k, scale)):
            total = jnp.sum(jnp.sum(value, axis=0, keepdims=True), axis=1, keepdims=True)
            row = jnp.where(lane_of == lane, total, row)
        stats[...] = row

    lane_of = lax.broadcasted_iota(jnp.int32, (1, width), 1)
    stats[...] = jnp.zeros_like(stats)
    for part in range(PARTS):
        loaded(*tiles[0], part)
        if len(tiles) > 2:
            load(*tiles[2], part)
        prepare_tile(at_tile(*tiles[0]), part)
    for copy in small:
        copy.wait()
    set_up()
    last = len(tiles) - 1
    ahead = me < EARLY

    def meet(n, ready):
        def go():
            pl.semaphore_wait(barrier, devices - 1)

        def pass_on(some):
            for f, t in some:
                send(0, f, t)
                send_rest(0, f, t)

        @pl.when(jnp.logical_not(ahead))
        def _():
            if n == 0:
                go()
            pass_on(ready)
            if n == 0:
                prior_copy.start()

        if n == last:
            @pl.when(ahead)
            def _():
                go()
                pass_on(tiles)
                prior_copy.start()

    for n, (f, t) in enumerate(tiles):
        if n > 0:
            for part in range(PARTS):
                loaded(f, t, part)
                if n + 2 < len(tiles):
                    load(*tiles[n + 2], part)
                prepare_tile(at_tile(f, t), part)
        tile_terms(0, f, t)
        meet(n, [(f, t)])

    for f, t in tiles:
        if f > 0:
            for c in range(2):
                prev[at_tile(f, t), c] = gain[at_tile(f - 1, t), c] * coef[3]

    def take_prior():
        prior_copy.wait_recv()
        for t in range(ttiles):
            i = at_tile(0, t)
            for c in range(2):
                for n in range(nb):
                    prev[i, c, n : n + 1, :] = from_prior[
                        t, c : c + 1, n * width : (n + 1) * width
                    ]
                prev[i, c] = prev[i, c] * coef[3]

    def step(k, carry):
        change, scale = zero, zero
        for f, t in tiles:
            arrived(k, f, t)
            if f == 0 and t == 0:
                pl.when(k == 0)(take_prior)
            change, scale = update(k, f, t, change, scale)
            tile_terms(k + 1, f, t)
            send(k + 1, f, t)
            send_rest(k + 1, f, t)
        record(k, change, scale)
        return carry

    lax.fori_loop(0, ITERS - 1, step, 0)
    change, scale = zero, zero
    for f, t in tiles:
        arrived(ITERS - 1, f, t)
        change, scale = update(ITERS - 1, f, t, change, scale)
    record(ITERS - 1, change, scale)

    def stats_copy(step, row):
        return pltpu.make_async_remote_copy(
            src_ref=stats, dst_ref=all_stats_ref.at[row],
            send_sem=stats_send.at[0], recv_sem=stats_recv.at[0],
            device_id=peer(step), device_id_type=LOGICAL,
        )

    def send_stats(step, carry):
        stats_copy(step, me).start()
        return carry

    lax.fori_loop(1, devices, send_stats, 0, unroll=UNROLL)
    own_stats = pltpu.make_async_copy(stats, all_stats_ref.at[me], out_sem.at[1])
    own_stats.start()
    prior_copy.wait_send()
    for f, t in tiles:
        i = at_tile(f, t)
        for c in range(2):
            for n in range(nb):
                prior_ref[f, t, c : c + 1, n * width : (n + 1) * width] = gain[i, c, n : n + 1, :]
    gains_out = pltpu.make_async_copy(prior_ref, gains_ref, out_sem.at[0])
    gains_out.start()

    wait_for(halo, halo_send.at[0])
    pl.when(ti < nt - 1)(lambda: wait_for(early, early_send.at[0]))
    pl.when(ti > 0)(lambda: wait_for(late, late_send.at[0]))
    own_stats.wait()
    gains_out.wait()
    others = all_stats_ref.at[pl.ds(0, devices - 1)]
    wait_for(others, stats_send.at[0])
    wait_for(others, stats_recv.at[0])


def hand_on(gains_in, stats_in, gains_ref, changes_ref):
    gains_ref[...] = gains_in[...]
    whole = jnp.sum(stats_in[...], axis=0)
    scale = pltpu.roll(whole, whole.shape[1] - ITERS, axis=1)
    changes_ref[...] = jnp.sqrt(whole / (scale + 1e-06))[0, :ITERS]


def per_device(vis, model, block_rows, block_cols, flags, prior, couplings, damping):
    nf, nt = lax.axis_size("freq"), lax.axis_size("tm")
    ftiles, ttiles, blks = vis.shape[:3]
    width = vis.shape[-1]
    nb = prior.shape[-1] // width
    count = ftiles * ttiles
    dims = (nf, nt, ftiles, ttiles, blks, width, nb)
    vmem = pl.BlockSpec(memory_space=pltpu.VMEM)
    hbm = pl.BlockSpec(memory_space=pltpu.HBM)
    dma = pltpu.SemaphoreType.DMA
    gains, all_stats = pl.pallas_call(
        functools.partial(kernel, dims),
        name="stefcal",
        out_shape=(
            jax.ShapeDtypeStruct(prior.shape, F32),
            jax.ShapeDtypeStruct((nf * nt, 1, width), F32),
        ),
        in_specs=[hbm] * 8,
        out_specs=(hbm, hbm),
        scratch_shapes=[
            pltpu.SMEM(block_rows.shape, jnp.int32),
            pltpu.SMEM(block_rows.shape, jnp.int32),
            pltpu.SMEM(block_rows.shape, jnp.int32),
            pltpu.VMEM(prior.shape, F32),
            pltpu.VMEM(couplings.shape, F32),
            pltpu.VMEM((1, damping.shape[0]), F32),
            pltpu.VMEM((count, 2) + vis.shape[2:], BF16),
            pltpu.VMEM((count, blks, 2, 2 * width, width), BF16),
            pltpu.VMEM((count, blks // 2, 2, 2 * width, width), BF16),
            pltpu.VMEM((count, 2, nb, width), F32),
            pltpu.VMEM((count, 2, nb, width), F32),
            pltpu.VMEM((4, nb, width), F32),
            pltpu.VMEM(prior.shape[1:], F32),
            pltpu.VMEM((ITERS, count, 3, nb, width), F32),
            pltpu.VMEM((ITERS, ttiles, 2 * REACH, 3, nb, width), F32),
            pltpu.VMEM((ITERS, ftiles, 3, nb, width), F32),
            pltpu.VMEM((ITERS, ftiles, 3, nb, width), F32),
            pltpu.VMEM((1, width), F32),
            dma((6,)),
            dma((count, PARTS)),
            dma((2,)),
            dma((1,)),
            dma((ITERS, ttiles, 2)),
            dma((1,)),
            dma((1,)),
            dma((ITERS,)),
            dma((ITERS,)),
            dma((1,)),
            dma((1,)),
            dma((2,)),
        ],
        compiler_params=pltpu.CompilerParams(
            collective_id=0, has_side_effects=True, vmem_limit_bytes=67043328
        ),
    )(vis, model, block_rows, block_cols, flags, prior, couplings, damping.reshape(1, -1))
    return pl.pallas_call(
        hand_on,
        name="hand_on",
        out_shape=(
            jax.ShapeDtypeStruct(prior.shape, F32),
            jax.ShapeDtypeStruct((ITERS,), F32),
        ),
        in_specs=[vmem, vmem],
        out_specs=(vmem, vmem),
    )(gains, all_stats)


def solution(mesh):
    placed = (
        P("freq", "tm", None, None, None, None),
        P("freq", "tm", None, None, None, None),
        P("freq", "tm", None),
        P("freq", "tm", None),
        P("freq", "tm", None),
        P("freq", "tm", None, None),
        P(),
        P(),
    )
    return jax.shard_map(
        per_device,
        mesh=mesh,
        in_specs=placed,
        out_specs=(P("freq", "tm", None, None), P()),
        check_vma=False,
    )
```

```python
import functools

import jax
import jax.numpy as jnp
from jax import lax
from jax.experimental import pallas as pl
from jax.experimental.pallas import tpu as pltpu
from jax.sharding import PartitionSpec as P

ITERS = 4
REACH = 2
EARLY = 2
UNROLL = 31
CHUNK = 16
PARTS = 4
MESH = pl.DeviceIdType.MESH
LOGICAL = pl.DeviceIdType.LOGICAL
F32 = jnp.float32
BF16 = jnp.bfloat16


def split(value):
    high = value.astype(BF16)
    return high, (value - high.astype(F32)).astype(BF16)


def kernel(
    dims,
    vis_ref, model_ref, rows_in, cols_in, flags_in, prior_in, coup_in, damp_in,
    gains_ref, all_stats_ref,
    rows_ref, cols_ref, flags_ref, prior_ref, coup_ref, damp_ref,
    data, wa, wb, gain, prev, coef, from_prior, terms, halo, early, late,
    stats,
    small_sem, load_sem, prior_sem, halo_send, halo_recv,
    early_send, late_send, early_recv, late_recv, stats_send, stats_recv, out_sem,
):
    nf, nt, ftiles, ttiles, blks, width, nb = dims
    fi = lax.axis_index("freq")
    ti = lax.axis_index("tm")
    above, below = lax.rem(fi + 1, nf), lax.rem(fi + nf - 1, nf)
    order = range(ftiles - 1, -1, -1)
    tiles = [(f, t) for t in range(ttiles) for f in order]

    def at_tile(f, t):
        return t * ftiles + f

    devices = nf * nt
    me = fi * nt + ti

    def peer(step):
        return lax.rem(me + step, devices)

    def parts(f, t):
        return PARTS if (f, t) == tiles[0] else 1

    def load(f, t, part):
        i, size = at_tile(f, t), blks // parts(f, t)
        some = pl.ds(part * size, size)
        for n, ref in enumerate((vis_ref, model_ref)):
            pltpu.make_async_copy(
                ref.at[f, t, some], data.at[i, n, some], load_sem.at[part if (f, t) == tiles[0] else PARTS + i]
            ).start()

    def loaded(f, t, part):
        i, size = at_tile(f, t), blks // parts(f, t)
        some = pl.ds(part * size, size)
        wait_for(data.at[i, :, some], load_sem.at[part if (f, t) == tiles[0] else PARTS + i])

    def wait_for(ref, sem):
        pltpu.make_async_copy(ref, ref, sem).wait()

    small = [
        pltpu.make_async_copy(src, dst, small_sem.at[n])
        for n, (src, dst) in enumerate((
            (prior_in, prior_ref), (coup_in, coup_ref), (damp_in, damp_ref),
            (rows_in, rows_ref), (cols_in, cols_ref), (flags_in, flags_ref),
        ))
    ]
    for copy in small:
        copy.start()
    for f, t in tiles[:2]:
        for part in range(parts(f, t)):
            load(f, t, part)

    barrier = pltpu.get_barrier_semaphore()

    def greet(step, carry):
        pl.semaphore_signal(barrier, inc=1, device_id=peer(step), device_id_type=LOGICAL)
        return carry

    lax.fori_loop(1, devices, greet, 0, unroll=UNROLL)

    def set_up():
        for f, t in tiles:
            i = at_tile(f, t)
            for c in range(2):
                for n in range(nb):
                    gain[i, c, n : n + 1, :] = prior_ref[f, t, c : c + 1, n * width : (n + 1) * width]
        for n in range(nb):
            for c in range(3):
                coef[c, n : n + 1, :] = coup_ref[c : c + 1, n * width : (n + 1) * width]
            coef[3, n : n + 1, :] = damp_ref[0:1, n * width : (n + 1) * width]

    prior_copy = pltpu.make_async_remote_copy(
        src_ref=prior_ref.at[ftiles - 1], dst_ref=from_prior,
        send_sem=prior_sem.at[0], recv_sem=prior_sem.at[1],
        device_id={"freq": above}, device_id_type=MESH,
    )

    def up_copy(k, f, t):
        return pltpu.make_async_remote_copy(
            src_ref=terms.at[k, at_tile(f, t)], dst_ref=halo.at[k, t, f - (ftiles - REACH)],
            send_sem=halo_send.at[0], recv_sem=halo_recv.at[k, t, int(f == ftiles - REACH)],
            device_id={"freq": above}, device_id_type=MESH,
        )

    def down_copy(k, f, t):
        return pltpu.make_async_remote_copy(
            src_ref=terms.at[k, at_tile(f, t)], dst_ref=halo.at[k, t, REACH + f],
            send_sem=halo_send.at[0], recv_sem=halo_recv.at[k, t, 0],
            device_id={"freq": below}, device_id_type=MESH,
        )

    def later_copy(k, f):
        return pltpu.make_async_remote_copy(
            src_ref=terms.at[k, at_tile(f, ttiles - 1)], dst_ref=early.at[k, f],
            send_sem=early_send.at[0], recv_sem=early_recv.at[k],
            device_id={"tm": lax.rem(ti + 1, nt)}, device_id_type=MESH,
        )

    def earlier_copy(k, f):
        return pltpu.make_async_remote_copy(
            src_ref=terms.at[k, at_tile(f, 0)], dst_ref=late.at[k, f],
            send_sem=late_send.at[0], recv_sem=late_recv.at[k],
            device_id={"tm": lax.rem(ti + nt - 1, nt)}, device_id_type=MESH,
        )

    def prepare(i, b, slot, side):
        for r in range(0, width, CHUNK):
            at = pl.ds(r, CHUNK)
            v_re = data[i, 0, b, 0, at].astype(F32)
            v_im = data[i, 0, b, 1, at].astype(F32)
            m_re = data[i, 1, b, 0, at].astype(F32)
            m_im = data[i, 1, b, 1, at].astype(F32)
            re = v_re * m_re + v_im * m_im
            im = v_re * m_im - v_im * m_re
            sq = m_re * m_re + m_im * m_im
            lower = pl.ds(width + r, CHUNK)
            wa[i, 2 * slot + side, 0, at], wb[i, slot, side, at] = split(re)
            wa[i, 2 * slot + side, 0, lower], wb[i, slot, side, lower] = split(im)
            wa[i, 2 * slot + side, 1, at], wa[i, 2 * slot + side, 1, lower] = split(sq)

    def prepare_pair(i, p):
        for side in range(2):
            prepare(i, 2 * p + side, p, side)

    def prepare_tile(i, part, count):
        def pair(p, carry):
            prepare_pair(i, p)
            return carry

        size = blks // 2 // count
        lax.fori_loop(part * size, part * size + size, pair, 0)

    row_of = lax.broadcasted_iota(jnp.int32, (8, width), 0)
    block_of = lax.broadcasted_iota(jnp.int32, (nb, width), 0)
    zero = jnp.zeros((nb, width), F32)

    def column(f, t, b):
        return jnp.where(flags_ref[f, t, b] != 0, cols_ref[f, t, b], -1)

    def gains_of(f, t, b):
        row, i = rows_ref[f, t, b], at_tile(f, t)
        return gain[i, 0, pl.ds(row, 1), :], gain[i, 1, pl.ds(row, 1), :]

    def add(total, col, parts):
        hit = block_of == col
        return [
            acc + jnp.where(hit, jnp.broadcast_to(one, (nb, width)), 0.0)
            for acc, one in zip(total, parts)
        ]

    def pair_terms(f, t, p, total):
        i = at_tile(f, t)
        highs, outs, cols = [], [], []
        for side in range(2):
            b = 2 * p + side
            cols.append(column(f, t, b))
            re, im = (jnp.broadcast_to(x, (8, width)) for x in gains_of(f, t, b))
            sq = re * re + im * im
            left = jnp.where(row_of == 0, re, jnp.where(row_of == 1, im, sq))
            right = jnp.where(row_of == 0, -im, jnp.where(row_of == 1, re, sq))
            lhs = jnp.concatenate([left, right], axis=1)
            lhs_hi = lhs.astype(BF16).astype(F32)
            highs.append(lhs_hi)
            lhs = jnp.concatenate([lhs_hi, lhs - lhs_hi], axis=0).astype(BF16)
            rhs = jnp.concatenate([wa[i, b, 0], wa[i, b, 1]], axis=1)
            out = jnp.dot(lhs, rhs, preferred_element_type=F32)
            outs.append(out[0:8] + out[8:16])
        low_out = jnp.dot(
            jnp.concatenate(highs, axis=0).astype(BF16),
            jnp.concatenate([wb[i, p, 0], wb[i, p, 1]], axis=1),
            preferred_element_type=F32,
        )
        low_outs = (low_out[0:8, 0:width], low_out[8:16, width:])
        for out, low_out, col in zip(outs, low_outs, cols):
            num = out[:, 0:width] + low_out
            total = add(total, col, (num[0:1], num[1:2], out[2:3, width:]))
        return total

    def keep(k, f, t, total):
        for c in range(3):
            terms[k, at_tile(f, t), c] = total[c]

    def tile_terms(k, f, t):
        total = [zero] * 3
        for p in range(blks // 2):
            total = pair_terms(f, t, p, total)
        keep(k, f, t, total)

    outer = lax.rem(fi, 2) == 1

    def send_up(k, f, t):
        if f >= ftiles - REACH:
            up_copy(k, f, t).start()

    def send_down(k, f, t):
        if f < REACH:
            down_copy(k, f, t).start()

    def send(k, f, t):
        if t == ttiles - 1:
            pl.when(ti < nt - 1)(later_copy(k, f).start)
        if t == 0:
            pl.when(ti > 0)(earlier_copy(k, f).start)
        pl.when(outer)(lambda: send_up(k, f, t))
        pl.when(jnp.logical_not(outer))(lambda: send_down(k, f, t))

    def send_rest(k, f, t):
        pl.when(outer)(lambda: send_down(k, f, t))
        pl.when(jnp.logical_not(outer))(lambda: send_up(k, f, t))

    def arrived(k, f, t):
        if f == ftiles - 1:
            if t == 0:
                pl.when(ti > 0)(lambda: wait_for(early.at[k], early_recv.at[k]))
            if t == ttiles - 1:
                pl.when(ti < nt - 1)(lambda: wait_for(late.at[k], late_recv.at[k]))
            wait_for(halo.at[k, t, pl.ds(1, 2 * REACH - 1)], halo_recv.at[k, t, 0])
        if f == 0:
            wait_for(halo.at[k, t, 0], halo_recv.at[k, t, 1])

    def update(k, f, t, change, scale):
        def at(f, t, c):
            if t < 0:
                return jnp.where(ti > 0, early[k, f, c], 0.0)
            if t >= ttiles:
                return jnp.where(ti < nt - 1, late[k, f, c], 0.0)
            if f < 0:
                return halo[k, t, f + REACH, c]
            if f >= ftiles:
                return halo[k, t, f - ftiles + REACH, c]
            return terms[k, at_tile(f, t), c]

        odd = lax.rem(k, 2) == 1
        i = at_tile(f, t)
        sums = [
            at(f, t, c)
            + coef[0] * (at(f - 1, t, c) + at(f + 1, t, c))
            + coef[1] * (at(f - 2, t, c) + at(f + 2, t, c))
            + coef[2] * (at(f, t - 1, c) + at(f, t + 1, c))
            for c in range(3)
        ]
        denom = sums[2] + coef[3]
        for c in range(2):
            old = gain[i, c]
            fresh = (sums[c] + prev[i, c]) / denom
            fresh = jnp.where(odd, 0.5 * (fresh + old), fresh)
            diff = fresh - old
            change = change + diff * diff
            scale = scale + fresh * fresh
            gain[i, c] = fresh
        return change, scale

    def record(k, change, scale):
        row = stats[...]
        for lane, value in ((k, change), (ITERS + k, scale)):
            total = jnp.sum(jnp.sum(value, axis=0, keepdims=True), axis=1, keepdims=True)
            row = jnp.where(lane_of == lane, total, row)
        stats[...] = row

    lane_of = lax.broadcasted_iota(jnp.int32, (1, width), 1)
    stats[...] = jnp.zeros_like(stats)
    for part in range(PARTS):
        loaded(*tiles[0], part)
        if part == 0 and len(tiles) > 2:
            load(*tiles[2], 0)
        prepare_tile(at_tile(*tiles[0]), part, PARTS)
    for copy in small:
        copy.wait()
    set_up()
    last = len(tiles) - 1
    ahead = me < EARLY

    def meet(n, ready):
        def go():
            pl.semaphore_wait(barrier, devices - 1)

        def pass_on(some):
            for f, t in some:
                send(0, f, t)
                send_rest(0, f, t)

        @pl.when(jnp.logical_not(ahead))
        def _():
            if n == 0:
                go()
            pass_on(ready)
            if n == 0:
                prior_copy.start()

        if n == last:
            @pl.when(ahead)
            def _():
                go()
                pass_on(tiles)
                prior_copy.start()

    for n, (f, t) in enumerate(tiles):
        if n > 0:
            loaded(f, t, 0)
            if n + 2 < len(tiles):
                load(*tiles[n + 2], 0)
            prepare_tile(at_tile(f, t), 0, 1)
        tile_terms(0, f, t)
        meet(n, [(f, t)])

    for f, t in tiles:
        if f > 0:
            for c in range(2):
                prev[at_tile(f, t), c] = gain[at_tile(f - 1, t), c] * coef[3]

    def take_prior():
        prior_copy.wait_recv()
        for t in range(ttiles):
            i = at_tile(0, t)
            for c in range(2):
                for n in range(nb):
                    prev[i, c, n : n + 1, :] = from_prior[
                        t, c : c + 1, n * width : (n + 1) * width
                    ]
                prev[i, c] = prev[i, c] * coef[3]

    def step(k, carry):
        change, scale = zero, zero
        for f, t in tiles:
            arrived(k, f, t)
            if f == 0 and t == 0:
                pl.when(k == 0)(take_prior)
            change, scale = update(k, f, t, change, scale)
            tile_terms(k + 1, f, t)
            send(k + 1, f, t)
            send_rest(k + 1, f, t)
        record(k, change, scale)
        return carry

    lax.fori_loop(0, ITERS - 1, step, 0)
    change, scale = zero, zero
    for f, t in tiles:
        arrived(ITERS - 1, f, t)
        change, scale = update(ITERS - 1, f, t, change, scale)
    record(ITERS - 1, change, scale)

    def stats_copy(step, row):
        return pltpu.make_async_remote_copy(
            src_ref=stats, dst_ref=all_stats_ref.at[row],
            send_sem=stats_send.at[0], recv_sem=stats_recv.at[0],
            device_id=peer(step), device_id_type=LOGICAL,
        )

    def send_stats(step, carry):
        stats_copy(step, me).start()
        return carry

    lax.fori_loop(1, devices, send_stats, 0, unroll=UNROLL)
    own_stats = pltpu.make_async_copy(stats, all_stats_ref.at[me], out_sem.at[1])
    own_stats.start()
    prior_copy.wait_send()
    for f, t in tiles:
        i = at_tile(f, t)
        for c in range(2):
            for n in range(nb):
                prior_ref[f, t, c : c + 1, n * width : (n + 1) * width] = gain[i, c, n : n + 1, :]
    gains_out = pltpu.make_async_copy(prior_ref, gains_ref, out_sem.at[0])
    gains_out.start()

    wait_for(halo, halo_send.at[0])
    pl.when(ti < nt - 1)(lambda: wait_for(early, early_send.at[0]))
    pl.when(ti > 0)(lambda: wait_for(late, late_send.at[0]))
    own_stats.wait()
    gains_out.wait()
    others = all_stats_ref.at[pl.ds(0, devices - 1)]
    wait_for(others, stats_send.at[0])
    wait_for(others, stats_recv.at[0])


def hand_on(gains_in, stats_in, gains_ref, changes_ref):
    gains_ref[...] = gains_in[...]
    whole = jnp.sum(stats_in[...], axis=0)
    scale = pltpu.roll(whole, whole.shape[1] - ITERS, axis=1)
    changes_ref[...] = jnp.sqrt(whole / (scale + 1e-06))[0, :ITERS]


def per_device(vis, model, block_rows, block_cols, flags, prior, couplings, damping):
    nf, nt = lax.axis_size("freq"), lax.axis_size("tm")
    ftiles, ttiles, blks = vis.shape[:3]
    width = vis.shape[-1]
    nb = prior.shape[-1] // width
    count = ftiles * ttiles
    dims = (nf, nt, ftiles, ttiles, blks, width, nb)
    vmem = pl.BlockSpec(memory_space=pltpu.VMEM)
    hbm = pl.BlockSpec(memory_space=pltpu.HBM)
    dma = pltpu.SemaphoreType.DMA
    gains, all_stats = pl.pallas_call(
        functools.partial(kernel, dims),
        name="stefcal",
        out_shape=(
            jax.ShapeDtypeStruct(prior.shape, F32),
            jax.ShapeDtypeStruct((nf * nt, 1, width), F32),
        ),
        in_specs=[hbm] * 8,
        out_specs=(hbm, hbm),
        scratch_shapes=[
            pltpu.SMEM(block_rows.shape, jnp.int32),
            pltpu.SMEM(block_rows.shape, jnp.int32),
            pltpu.SMEM(block_rows.shape, jnp.int32),
            pltpu.VMEM(prior.shape, F32),
            pltpu.VMEM(couplings.shape, F32),
            pltpu.VMEM((1, damping.shape[0]), F32),
            pltpu.VMEM((count, 2) + vis.shape[2:], BF16),
            pltpu.VMEM((count, blks, 2, 2 * width, width), BF16),
            pltpu.VMEM((count, blks // 2, 2, 2 * width, width), BF16),
            pltpu.VMEM((count, 2, nb, width), F32),
            pltpu.VMEM((count, 2, nb, width), F32),
            pltpu.VMEM((4, nb, width), F32),
            pltpu.VMEM(prior.shape[1:], F32),
            pltpu.VMEM((ITERS, count, 3, nb, width), F32),
            pltpu.VMEM((ITERS, ttiles, 2 * REACH, 3, nb, width), F32),
            pltpu.VMEM((ITERS, ftiles, 3, nb, width), F32),
            pltpu.VMEM((ITERS, ftiles, 3, nb, width), F32),
            pltpu.VMEM((1, width), F32),
            dma((6,)),
            dma((PARTS + count,)),
            dma((2,)),
            dma((1,)),
            dma((ITERS, ttiles, 2)),
            dma((1,)),
            dma((1,)),
            dma((ITERS,)),
            dma((ITERS,)),
            dma((1,)),
            dma((1,)),
            dma((2,)),
        ],
        compiler_params=pltpu.CompilerParams(
            collective_id=0, has_side_effects=True, vmem_limit_bytes=67043328
        ),
    )(vis, model, block_rows, block_cols, flags, prior, couplings, damping.reshape(1, -1))
    return pl.pallas_call(
        hand_on,
        name="hand_on",
        out_shape=(
            jax.ShapeDtypeStruct(prior.shape, F32),
            jax.ShapeDtypeStruct((ITERS,), F32),
        ),
        in_specs=[vmem, vmem],
        out_specs=(vmem, vmem),
    )(gains, all_stats)


def solution(mesh):
    placed = (
        P("freq", "tm", None, None, None, None),
        P("freq", "tm", None, None, None, None),
        P("freq", "tm", None),
        P("freq", "tm", None),
        P("freq", "tm", None),
        P("freq", "tm", None, None),
        P(),
        P(),
    )
    return jax.shard_map(
        per_device,
        mesh=mesh,
        in_specs=placed,
        out_specs=(P("freq", "tm", None, None), P()),
        check_vma=False,
    )
```
